32 devices in a mesh: grp: 4 (over z), elem: 8 (over y, x, core).
Axes of the slice: x: 2, y: 2, z: 4, core: 2. Of those that a mesh axis runs over, the one named last changes fastest.
Arguments:
- velocity: float32 [3, 343, 4096], P(None, None, ('grp', 'elem')), may hold values from -0.6 to 0.6
- adjoint: float32 [3, 343, 4096], P(None, None, ('grp', 'elem')), may hold values from -0.6 to 0.6
- spacing: float32 [3, 4096], P(None, ('grp', 'elem')), may hold values from 0.5 to 2
- elem_count: int32 [32], P(('grp', 'elem')), may hold values from 32 to 128, as said below
- design_map: int32 [8, 4096], P(None, ('grp', 'elem')), may hold values from 0 to 65535, as said below
Outputs:
- direction: float32 [3, 65536], P(None, ('grp', 'elem'))
- objective: float32 [], replicated
The draws below stay inside these ranges and needn't reach their ends.
Inputs may be any that keep to these rules, and one draw needn't show every extreme that they name: `elem_count`: the largest count equals 128 in every draw. `design_map`: design node d belongs to the device numbered d // 2048, counting grp first and elem second. Every entry of a device's columns names a node of a device whose elem index differs from that device's by at most one, cyclically over the elem axis, in any group.
All inputs are finite; a program needn't handle non-finite values.
Results may differ from the reference program's by a relative error of at most 0.0003.
Values sent between devices are 32-bit elements; how exact they have to be, the bound alone decides.
A program may use at most 64 MiB of HBM per device.

```python
import math
import jax
import jax.numpy as jnp
import numpy as np
from jax import lax

P_SIZE = 7
ELEM_DEV = 128
ND_DEV = 2048
ELEMS = 4096
N_GRP = 4
N_ELEM = 8


def node_field(key, salt):
    elements = ELEM_DEV * N_GRP * N_ELEM
    seeded = jax.random.fold_in(key, salt)
    jitter_key, shared_key = jax.random.split(seeded)
    shared_part = jnp.clip(jax.random.normal(shared_key, (3, P_SIZE ** 3, 1), jnp.float32), -4.0, 4.0)
    jitter_part = jnp.clip(jax.random.normal(jitter_key, (3, P_SIZE ** 3, elements), jnp.float32), -4.0, 4.0)
    return 0.07 * shared_part + 0.07 * jitter_part


def draw_velocity(key, part):
    return node_field(key, 11)


def draw_adjoint(key, part):
    return node_field(key, 23)


def draw_elem_count(key, part):
    devices = N_GRP * N_ELEM
    index = jnp.arange(devices, dtype=jnp.int32)
    base = ELEM_DEV // 3 + index * (ELEM_DEV - ELEM_DEV // 3) // (devices - 1)
    jitter = jax.random.randint(key, (devices,), 0, max(ELEM_DEV // 16, 2), dtype=jnp.int32)
    jitter = jnp.where(index == devices - 1, 0, jitter)
    return (base - jitter).astype(jnp.int32)


def draw_design_map(key, part):
    devices = N_GRP * N_ELEM
    total = ELEM_DEV * devices
    column = jnp.arange(total, dtype=jnp.int32)
    device = column // ELEM_DEV
    home_grp = (device // N_ELEM)[None, :]
    home_col = (device % N_ELEM)[None, :]
    first, second, third, fourth = jax.random.split(key, 4)
    same = jax.random.randint(first, (8, total), 0, 2, dtype=jnp.int32)
    other = jax.random.randint(second, (8, total), 1, N_GRP, dtype=jnp.int32)
    owner_grp = jnp.where(same == 1, home_grp, (home_grp + other) % N_GRP)
    offset = jax.random.randint(third, (8, total), -1, 2, dtype=jnp.int32)
    owner_col = (home_col + offset + N_ELEM) % N_ELEM
    vertex_ids = jnp.arange(8, dtype=jnp.int32)[:, None]
    within = 8 * jax.random.randint(fourth, (8, total), 0, ND_DEV // 8, dtype=jnp.int32) + vertex_ids
    return ((owner_grp * N_ELEM + owner_col) * ND_DEV + within).astype(jnp.int32)


def levels(stream_key, shape, cuts, low, top_value):
    factor_of = 1.0
    for position, blocks in cuts:
        draws = jax.random.uniform(jax.random.fold_in(jax.random.fold_in(stream_key, 6), position), (blocks,), jnp.float32, low / len(cuts), top_value / len(cuts))
        factor_of = factor_of * jnp.repeat(jnp.exp(draws), shape[position] // blocks).reshape((-1,) + (1,) * (len(shape) - 1 - position))
    return factor_of


def setup_inputs(seed: int = 0) -> dict:
    keys = jax.random.split(jax.random.key(seed), 6)
    velocity = draw_velocity(jax.random.fold_in(keys[5], 71), 0)
    adjoint = draw_adjoint(jax.random.fold_in(keys[5], 71), 0)
    spacing = jnp.clip(jnp.exp(math.log(2.0) - 1.3862944 * jax.random.uniform(keys[2], (3, ELEMS), jnp.float32) ** levels(keys[2], (3, ELEMS), ((1, 32),), -0.2, 0.2)), 0.5, 2.0)
    elem_count = draw_elem_count(jax.random.fold_in(keys[5], 71), 0)
    design_map = draw_design_map(jax.random.fold_in(keys[5], 71), 0)
    return {"velocity": velocity, "adjoint": adjoint, "spacing": spacing, "elem_count": elem_count, "design_map": design_map}


def lobatto(degree):
    points = np.cos(np.pi * np.arange(degree + 1) / degree)
    for sweep in range(60):
        lower = np.ones(degree + 1)
        upper = points.copy()
        for order in range(2, degree + 1):
            lower, upper = (upper, ((2 * order - 1) * points * upper - (order - 1) * lower) / order)
        points = points - (points * upper - lower) / ((degree + 1) * upper)
    lower = np.ones(degree + 1)
    upper = points.copy()
    for order in range(2, degree + 1):
        lower, upper = (upper, ((2 * order - 1) * points * upper - (order - 1) * lower) / order)
    return (points[::-1].copy(), upper[::-1].copy())

def tables():
    degree = P_SIZE - 1
    points, values = lobatto(degree)
    weights = 2.0 / (degree * (degree + 1) * values ** 2)
    derivative = np.zeros((P_SIZE, P_SIZE))
    for i in range(P_SIZE):
        for j in range(P_SIZE):
            if i != j:
                derivative[i, j] = values[i] / (values[j] * (points[i] - points[j]))
    derivative[0, 0] = -degree * (degree + 1) / 4.0
    derivative[P_SIZE - 1, P_SIZE - 1] = degree * (degree + 1) / 4.0
    coords = np.meshgrid(points, points, points, indexing='ij')
    coords = [c.reshape(-1) for c in coords]
    spread = np.meshgrid(weights, weights, weights, indexing='ij')
    quadrature = (spread[0] * spread[1] * spread[2]).reshape(-1)
    vertex_grad = np.zeros((3, 8, P_SIZE ** 3))
    for vertex in range(8):
        signs = [2.0 * (vertex >> 2 - m & 1) - 1.0 for m in range(3)]
        factors = [(1.0 + signs[m] * coords[m]) / 2.0 for m in range(3)]
        for j in range(3):
            others = [factors[m] for m in range(3) if m != j]
            vertex_grad[j, vertex] = signs[j] / 2.0 * others[0] * others[1] * quadrature
    return (jnp.asarray(derivative, jnp.float32), jnp.asarray(vertex_grad, jnp.float32), jnp.asarray(quadrature, jnp.float32))

def element_terms(velocity, adjoint, spacing, derivative, vertex_grad, quadrature):
    blocks = velocity.shape[-1]
    factor = 2.0 / spacing
    jacobian = spacing[0] * spacing[1] * spacing[2] / 8.0
    highest = lax.Precision.HIGHEST

    def gradient(field):
        cube = field.reshape(3, P_SIZE, P_SIZE, P_SIZE, blocks)
        first = jnp.einsum('ij,cjklb->ciklb', derivative, cube, precision=highest)
        second = jnp.einsum('ij,ckjlb->ckilb', derivative, cube, precision=highest)
        third = jnp.einsum('ij,ckljb->cklib', derivative, cube, precision=highest)
        stacked = jnp.stack([first, second, third], axis=1).reshape(3, 3, P_SIZE ** 3, blocks)
        return stacked * factor[None, :, None, :]
    grad_u = gradient(velocity)
    grad_w = gradient(adjoint)
    inner = lax.optimization_barrier(jnp.sum(grad_u * grad_w, axis=(0, 1)))
    cross = jnp.einsum('icqb,ijqb->cjqb', grad_u, grad_w, precision=highest)
    unit = jnp.eye(3, dtype=jnp.float32)
    stress = unit[:, :, None, None] * inner[None, None] - cross - jnp.swapaxes(cross, 0, 1)
    contrib = jnp.einsum('cjqb,jkq->cjkb', stress, vertex_grad, precision=highest)
    terms = lax.optimization_barrier(jnp.sum(contrib * factor[None, :, None, :], axis=1)) * jacobian[None, None, :]
    squared = lax.optimization_barrier(jnp.sum(grad_u * grad_u, axis=(0, 1)))
    dissipated = jacobian * jnp.einsum('qb,q->b', squared, quadrature, precision=highest)
    return (terms, dissipated)

def reference(velocity, adjoint, spacing, elem_count, design_map):
    devices = N_GRP * N_ELEM
    design_total = ND_DEV * devices
    derivative, vertex_grad, quadrature = tables()

    def one_device(carry, device):
        gradient_sum, spent = carry
        start = (device * ELEM_DEV).astype(jnp.int32)
        field_u = lax.dynamic_slice_in_dim(velocity, start, ELEM_DEV, 2)
        field_w = lax.dynamic_slice_in_dim(adjoint, start, ELEM_DEV, 2)
        lengths = lax.dynamic_slice_in_dim(spacing, start, ELEM_DEV, 1)
        nodes = lax.dynamic_slice_in_dim(design_map, start, ELEM_DEV, 1)
        terms, dissipated = element_terms(field_u, field_w, lengths, derivative, vertex_grad, quadrature)
        live = (jnp.arange(ELEM_DEV, dtype=jnp.int32) < elem_count[device]).astype(jnp.float32)
        terms = terms * live[None, None, :]
        gradient_sum = gradient_sum.at[:, nodes.reshape(-1)].add(terms.reshape(3, -1))
        return ((gradient_sum, spent + jnp.sum(dissipated * live)), None)
    init = (jnp.zeros((3, design_total), jnp.float32), jnp.zeros((), jnp.float32))
    (gradient_sum, spent), _ = lax.scan(one_device, init, jnp.arange(devices, dtype=jnp.int32))
    mean_square = jnp.sum(gradient_sum * gradient_sum) / (3.0 * design_total)
    direction = gradient_sum * lax.rsqrt(mean_square + 1e-06)
    objective = spent / (P_SIZE ** 3 * ELEM_DEV * devices)
    return (direction, objective)
```

```python
import functools

import jax
import jax.numpy as jnp
import numpy as np
from jax import lax
from jax.experimental import pallas as pl
from jax.experimental.pallas import tpu as pltpu
from jax.sharding import PartitionSpec as P

P_SIZE = 7
ND_DEV = 2048
LANES = 128
UPPER = ND_DEV // LANES
NODES = P_SIZE**3
ROWS = -(-NODES // 16) * 16
HEAD = 240
BACK = 192
TAIL = ROWS - HEAD
MESH = pl.DeviceIdType.MESH
F32 = jnp.float32
BF16 = jnp.bfloat16
VMEM_BYTES = 32 * 2**20


def lobatto(degree):
    points = np.cos(np.pi * np.arange(degree + 1) / degree)
    for sweep in range(60):
        lower = np.ones(degree + 1)
        upper = points.copy()
        for order in range(2, degree + 1):
            lower, upper = (upper, ((2 * order - 1) * points * upper - (order - 1) * lower) / order)
        points = points - (points * upper - lower) / ((degree + 1) * upper)
    lower = np.ones(degree + 1)
    upper = points.copy()
    for order in range(2, degree + 1):
        lower, upper = (upper, ((2 * order - 1) * points * upper - (order - 1) * lower) / order)
    return (points[::-1].copy(), upper[::-1].copy())


def halves(table):
    exact = np.asarray(table, np.float32)
    high = exact.astype(BF16)
    low = (exact - high.astype(np.float32)).astype(BF16)
    return (high, low)


def derivative_table():
    degree = P_SIZE - 1
    points, values = lobatto(degree)
    derivative = np.zeros((P_SIZE, P_SIZE))
    for i in range(P_SIZE):
        for j in range(P_SIZE):
            if i != j:
                derivative[i, j] = values[i] / (values[j] * (points[i] - points[j]))
    derivative[0, 0] = -degree * (degree + 1) / 4.0
    derivative[P_SIZE - 1, P_SIZE - 1] = degree * (degree + 1) / 4.0
    return derivative


def tables():
    degree = P_SIZE - 1
    points, values = lobatto(degree)
    weights = 2.0 / (degree * (degree + 1) * values**2)
    derivative = derivative_table()
    coords = np.meshgrid(points, points, points, indexing="ij")
    coords = [c.reshape(-1) for c in coords]
    spread = np.meshgrid(weights, weights, weights, indexing="ij")
    quadrature = (spread[0] * spread[1] * spread[2]).reshape(-1)
    contract = np.zeros((32, ROWS))
    for vertex in range(8):
        signs = [2.0 * (vertex >> 2 - m & 1) - 1.0 for m in range(3)]
        factors = [(1.0 + signs[m] * coords[m]) / 2.0 for m in range(3)]
        for j in range(3):
            others = [factors[m] for m in range(3) if m != j]
            contract[8 * j + vertex, :NODES] = signs[j] / 2.0 * others[0] * others[1] * quadrature
    contract[24, :NODES] = quadrature
    unit = np.eye(P_SIZE)
    near = np.zeros((2, ROWS, NODES))
    near[0, :NODES] = np.kron(np.kron(unit, derivative), unit)
    near[1, :NODES] = np.kron(np.kron(unit, unit), derivative)
    return (
        np.stack(halves(near[:, :HEAD, :256].reshape(2 * HEAD, 256))),
        np.stack(halves(near[:, HEAD:, BACK:].reshape(2 * TAIL, NODES - BACK))),
        np.concatenate(halves(contract)),
    )


def split(value):
    high = value.astype(BF16)
    return (high, (value - high.astype(F32)).astype(BF16))


def far_derivatives(velocity, adjoint, far):
    table = derivative_table()
    width = P_SIZE * P_SIZE
    for f, field in enumerate((velocity, adjoint)):
        for i in range(3):
            far[3 * f + i, ROWS - 16 :, :] = jnp.zeros((16, field.shape[2]), F32)
            slabs = [field[i, pl.ds(width * a, width), :] for a in range(P_SIZE)]
            for a in range(P_SIZE):
                far[3 * f + i, pl.ds(width * a, width), :] = sum(
                    float(table[a, b]) * slabs[b] for b in range(P_SIZE)
                )


def near_derivatives(fields, head, tail):
    high, low = split(fields)

    def apply(table, begin, end):
        return (
            jnp.dot(table[0], high[begin:end], preferred_element_type=F32)
            + jnp.dot(table[1], high[begin:end], preferred_element_type=F32)
            + jnp.dot(table[0], low[begin:end], preferred_element_type=F32)
        )

    upper = apply(head, 0, 256)
    lower = apply(tail, BACK, NODES)
    return [
        jnp.concatenate([upper[j * HEAD : (j + 1) * HEAD], lower[j * TAIL : (j + 1) * TAIL]], axis=0)
        for j in range(2)
    ]


def element_terms(far, near, spacing, live, contract):
    slots = spacing.shape[1]

    def grad(field, i, j):
        column = (3 * field + i) * slots
        return near[j - 1][:, column : column + slots] if j else far[3 * field + i]

    def product(c, j):
        return sum(grad(0, i, c) * grad(1, i, j) for i in range(3))

    pairs = [(0, 1), (0, 2), (1, 2)]
    stack = [product(m, m) for m in range(3)]
    stack += [product(c, j) + product(j, c) for c, j in pairs]
    stack += [sum(grad(0, i, j) * grad(0, i, j) for i in range(3)) for j in range(3)]
    stack_high, stack_low = split(jnp.concatenate(stack, axis=1))
    both = jnp.dot(contract, stack_high, preferred_element_type=F32)
    sums = both[:32] + both[32:] + jnp.dot(contract[:32], stack_low, preferred_element_type=F32)

    def part(j, column):
        return sums[8 * j : 8 * j + 8, column * slots : (column + 1) * slots]

    factor = [2.0 / spacing[j : j + 1] for j in range(3)]
    square = [f * f for f in factor]
    jacobian = spacing[0:1] * spacing[1:2] * spacing[2:3] * 0.125
    terms = []
    for c in range(3):
        total = sum(square[m] * part(c, m) for m in range(3)) - 2.0 * square[c] * part(c, c)
        for column, pair in enumerate(pairs):
            if c in pair:
                j = pair[0] + pair[1] - c
                total = total - square[j] * part(j, 3 + column)
        terms.append(jnp.where(live, total * (factor[c] * jacobian), 0.0))
    spent = sum(square[j] * part(3, 6 + j) for j in range(3)) * jacobian
    return (terms, jnp.where(live, spent, 0.0))


def place(index, rows, values=None):
    slots = index.shape[1]
    row = lax.broadcasted_iota(jnp.int32, (rows, slots), 0)
    columns = []
    for k in range(8):
        hit = row == index[k : k + 1]
        if values is None:
            columns.append(jnp.where(hit, 1.0, 0.0).astype(BF16))
        else:
            columns.append(
                jnp.concatenate(
                    [jnp.where(hit, v[k : k + 1], 0.0).astype(BF16) for v in values], axis=0
                )
            )
    return jnp.concatenate(columns, axis=1)


def far_first(groups, grp):
    place = jnp.minimum(grp, groups - 1 - grp)
    sign = 1 - 2 * (2 * grp // groups)
    single = groups - 1 - 2 * place
    steps = []
    for turn in range(groups - 1):
        rest = turn - single
        pair = (place - rest // 2) * (1 - 2 * lax.rem(rest + 2 * groups, 2))
        offset = jnp.where(rest < 0, groups - 1 - place - turn, pair)
        steps.append(lax.rem(sign * offset + groups, groups))
    return steps


def kernel(
    groups, columns,
    velocity_in, adjoint_in, spacing_in, count_in, map_in, head_in, tail_in, contract_in,
    direction, objective,
    velocity, adjoint, spacing, count, design_map, head, tail, contract, far,
    outgoing, maps, arrived, placed, gathered,
    local_sem, send_map, recv_map, send_sem, recv_sem, send_all, recv_all,
):
    devices = groups * columns
    grp, col = lax.axis_index("grp"), lax.axis_index("elem")
    me = grp * columns + col
    slots = spacing.shape[1]

    barrier = pltpu.get_barrier_semaphore()
    pairs = [
        (velocity_in, velocity), (adjoint_in, adjoint), (head_in, head), (tail_in, tail),
        (map_in, design_map), (spacing_in, spacing), (count_in, count), (contract_in, contract),
    ]
    loads = [pltpu.make_async_copy(a, b, local_sem.at[i]) for i, (a, b) in enumerate(pairs)]
    for load in loads:
        load.start()

    steps = far_first(groups, grp)

    def at(step, turn):
        return (lax.rem(grp + step, groups), lax.rem(col + turn, columns))

    everyone = [(step, turn) for step in steps for turn in range(columns)]
    everyone += [(0, turn) for turn in range(1, columns)]
    for step, turn in everyone:
        pl.semaphore_signal(barrier, inc=1, device_id=at(step, turn), device_id_type=MESH)
    for load in loads[:4]:
        load.wait()

    fields = jnp.concatenate([f[i] for f in (velocity, adjoint) for i in range(3)], axis=1)
    near = near_derivatives(fields, head, tail)
    far_derivatives(velocity, adjoint, far)

    for load in loads[4:]:
        load.wait()
    def copy(source, target, send, receive, o, step):
        slot = o * groups + step
        return pltpu.make_async_remote_copy(
            src_ref=source,
            dst_ref=target.at[slot],
            send_sem=send.at[slot],
            recv_sem=receive.at[slot],
            device_id=at(step, (o + columns - 1) % columns),
            device_id_type=MESH,
        )

    sends = [(o, step) for step in steps for o in (0, 2, 1)] + [(0, 0), (2, 0)]
    waits = [(o, step) for step in range(groups) for o in (1, 0, 2) if o != 1 or step]

    def map_copy(o, step):
        return copy(design_map, maps, send_map, recv_map, o, step)

    def term_copy(o, step):
        return copy(outgoing, arrived, send_sem, recv_sem, o, step)

    live = lax.broadcasted_iota(jnp.int32, (8, slots), 1) < count[0]
    terms, spent = element_terms(far, near, spacing[...], live, contract[...])
    for c in range(3):
        outgoing[8 * c : 8 * c + 8, :] = terms[c]
    pl.semaphore_wait(barrier, devices - 1)
    for o, step in sends:
        map_copy(o, step).start()
    for o, step in sends:
        term_copy(o, step).start()

    base = me * UPPER

    def collect(nodes, term, lower):
        index = lax.shift_right_logical(nodes, jnp.full_like(nodes, LANES.bit_length() - 1)) - base
        highs = [term[8 * c : 8 * c + 8].astype(BF16).astype(F32) for c in range(3)]
        lows = [term[8 * c : 8 * c + 8] - highs[c] for c in range(3)]
        return lax.dot_general(
            place(index, UPPER, highs + lows),
            lower,
            (((1,), (1,)), ((), ())),
            preferred_element_type=F32,
        )

    nodes = design_map[...]
    both = collect(nodes, outgoing[...], place(nodes & (LANES - 1), LANES))
    for o, step in waits:
        slot = o * groups + step
        map_copy(o, step).wait()
        placed[slot] = place(maps[slot] & (LANES - 1), LANES)

    for o, step in waits:
        slot = o * groups + step
        term_copy(o, step).wait_recv()
        both = both + collect(maps[slot], arrived[slot], placed[slot])
    total = both[: 3 * UPPER] + both[3 * UPPER :]

    squares = total * total
    squares = sum(squares[8 * i : 8 * i + 8] for i in range(3 * UPPER // 8))
    lane = lax.broadcasted_iota(jnp.int32, (8, LANES), 1)
    mixed = jnp.where(
        lane < LANES // 2,
        squares + pltpu.roll(squares, LANES // 2, 1),
        spent + pltpu.roll(spent, LANES // 2, 1),
    )
    gathered[devices - 1] = jnp.sum(mixed, axis=0, keepdims=True)

    def share(step, turn):
        slot = step * columns + turn - 1
        return pltpu.make_async_remote_copy(
            src_ref=gathered.at[devices - 1],
            dst_ref=gathered.at[slot],
            send_sem=send_all.at[slot],
            recv_sem=recv_all.at[slot],
            device_id=at(step, turn),
            device_id_type=MESH,
        )

    for step, turn in everyone:
        share(step, turn).start()
    for o, step in sends:
        term_copy(o, step).wait_send()
    for step, turn in everyone:
        share(step, turn).wait_recv()
    everything = jnp.sum(gathered[...], axis=0)
    first = lax.broadcasted_iota(jnp.int32, (1, LANES), 1) < LANES // 2
    square_total = jnp.sum(jnp.where(first, everything, 0.0), axis=1, keepdims=True)
    spent_total = jnp.sum(jnp.where(first, 0.0, everything), axis=1, keepdims=True)
    scale = lax.rsqrt(square_total * (1.0 / (3.0 * ND_DEV * devices)) + 1e-06)
    scaled = total * scale
    for c in range(3):
        direction[c] = scaled[UPPER * c : UPPER * c + UPPER]
    objective[...] = jnp.broadcast_to(spent_total * (1.0 / (NODES * slots * devices)), (1, LANES))
    for step, turn in everyone:
        share(step, turn).wait_send()


def hand_over(scaled, spent, direction, objective):
    for c in range(3):
        for u in range(UPPER):
            direction[c : c + 1, u * LANES : (u + 1) * LANES] = scaled[c, u : u + 1, :]
    objective[...] = spent[:, :1]


def body(groups, columns, velocity, adjoint, spacing, elem_count, design_map):
    devices = groups * columns
    blocks = 3 * groups
    slots = spacing.shape[1]
    vmem = pl.BlockSpec(memory_space=pltpu.VMEM)
    constants = tables()
    operands = [
        pltpu.with_memory_space_constraint(jnp.asarray(x), pltpu.HBM)
        for x in (velocity, adjoint, spacing)
    ]
    operands.append(elem_count)
    operands += [
        pltpu.with_memory_space_constraint(jnp.asarray(x), pltpu.HBM)
        for x in (design_map, *constants)
    ]
    scaled, spent = pl.pallas_call(
        functools.partial(kernel, groups, columns),
        out_shape=(
            jax.ShapeDtypeStruct((3, UPPER, LANES), F32),
            jax.ShapeDtypeStruct((1, LANES), F32),
        ),
        in_specs=[pl.BlockSpec(memory_space=pltpu.HBM)] * 8,
        out_specs=(vmem, vmem),
        scratch_shapes=[
            pltpu.VMEM(velocity.shape, F32),
            pltpu.VMEM(adjoint.shape, F32),
            pltpu.VMEM(spacing.shape, F32),
            pltpu.SMEM((1,), jnp.int32),
            pltpu.VMEM((8, slots), jnp.int32),
            *[pltpu.VMEM(table.shape, BF16) for table in constants],
            pltpu.VMEM((6, ROWS, slots), F32),
            pltpu.VMEM((24, slots), F32),
            pltpu.VMEM((blocks, 8, slots), jnp.int32),
            pltpu.VMEM((blocks, 24, slots), F32),
            pltpu.VMEM((blocks, LANES, 8 * slots), BF16),
            pltpu.VMEM((devices, 1, LANES), F32),
            pltpu.SemaphoreType.DMA((8,)),
            *[pltpu.SemaphoreType.DMA((blocks,))] * 4,
            *[pltpu.SemaphoreType.DMA((devices,))] * 2,
        ],
        compiler_params=pltpu.CompilerParams(
            collective_id=0, has_side_effects=True, vmem_limit_bytes=VMEM_BYTES
        ),
    )(*operands)
    direction, objective = pl.pallas_call(
        hand_over,
        out_shape=(
            jax.ShapeDtypeStruct((3, ND_DEV), F32),
            jax.ShapeDtypeStruct((1, 1), F32),
        ),
        in_specs=[vmem] * 2,
        out_specs=(vmem, vmem),
        compiler_params=pltpu.CompilerParams(vmem_limit_bytes=VMEM_BYTES),
    )(scaled, spent)
    return (direction, objective.reshape(()))


def solution(mesh):
    return jax.shard_map(
        functools.partial(body, mesh.shape["grp"], mesh.shape["elem"]),
        mesh=mesh,
        in_specs=(
            P(None, None, ("grp", "elem")),
            P(None, None, ("grp", "elem")),
            P(None, ("grp", "elem")),
            P(("grp", "elem")),
            P(None, ("grp", "elem")),
        ),
        out_specs=(P(None, ("grp", "elem")), P()),
        check_vma=False,
    )
```

```python
import functools

import jax
import jax.numpy as jnp
import numpy as np
from jax import lax
from jax.experimental import pallas as pl
from jax.experimental.pallas import tpu as pltpu
from jax.sharding import PartitionSpec as P

P_SIZE = 7
ND_DEV = 2048
LANES = 128
UPPER = ND_DEV // LANES
NODES = P_SIZE**3
ROWS = -(-NODES // 16) * 16
HEAD = 240
BACK = 192
TAIL = ROWS - HEAD
MESH = pl.DeviceIdType.MESH
F32 = jnp.float32
BF16 = jnp.bfloat16
VMEM_BYTES = 32 * 2**20


def lobatto(degree):
    points = np.cos(np.pi * np.arange(degree + 1) / degree)
    for sweep in range(60):
        lower = np.ones(degree + 1)
        upper = points.copy()
        for order in range(2, degree + 1):
            lower, upper = (upper, ((2 * order - 1) * points * upper - (order - 1) * lower) / order)
        points = points - (points * upper - lower) / ((degree + 1) * upper)
    lower = np.ones(degree + 1)
    upper = points.copy()
    for order in range(2, degree + 1):
        lower, upper = (upper, ((2 * order - 1) * points * upper - (order - 1) * lower) / order)
    return (points[::-1].copy(), upper[::-1].copy())


def halves(table):
    exact = np.asarray(table, np.float32)
    high = exact.astype(BF16)
    low = (exact - high.astype(np.float32)).astype(BF16)
    return (high, low)


def derivative_table():
    degree = P_SIZE - 1
    points, values = lobatto(degree)
    derivative = np.zeros((P_SIZE, P_SIZE))
    for i in range(P_SIZE):
        for j in range(P_SIZE):
            if i != j:
                derivative[i, j] = values[i] / (values[j] * (points[i] - points[j]))
    derivative[0, 0] = -degree * (degree + 1) / 4.0
    derivative[P_SIZE - 1, P_SIZE - 1] = degree * (degree + 1) / 4.0
    return derivative


def tables():
    degree = P_SIZE - 1
    points, values = lobatto(degree)
    weights = 2.0 / (degree * (degree + 1) * values**2)
    derivative = derivative_table()
    coords = np.meshgrid(points, points, points, indexing="ij")
    coords = [c.reshape(-1) for c in coords]
    spread = np.meshgrid(weights, weights, weights, indexing="ij")
    quadrature = (spread[0] * spread[1] * spread[2]).reshape(-1)
    contract = np.zeros((32, ROWS))
    for vertex in range(8):
        signs = [2.0 * (vertex >> 2 - m & 1) - 1.0 for m in range(3)]
        factors = [(1.0 + signs[m] * coords[m]) / 2.0 for m in range(3)]
        for j in range(3):
            others = [factors[m] for m in range(3) if m != j]
            contract[8 * j + vertex, :NODES] = signs[j] / 2.0 * others[0] * others[1] * quadrature
    contract[24, :NODES] = quadrature
    unit = np.eye(P_SIZE)
    near = np.zeros((2, ROWS, NODES))
    near[0, :NODES] = np.kron(np.kron(unit, derivative), unit)
    near[1, :NODES] = np.kron(np.kron(unit, unit), derivative)
    return (
        np.stack(halves(near[:, :HEAD, :256].reshape(2 * HEAD, 256))),
        np.stack(halves(near[:, HEAD:, BACK:].reshape(2 * TAIL, NODES - BACK))),
        np.concatenate(halves(contract)),
    )


def split(value):
    high = value.astype(BF16)
    return (high, (value - high.astype(F32)).astype(BF16))


def far_derivatives(velocity, adjoint, far):
    table = derivative_table()
    width = P_SIZE * P_SIZE
    for f, field in enumerate((velocity, adjoint)):
        for i in range(3):
            far[3 * f + i, ROWS - 16 :, :] = jnp.zeros((16, field.shape[2]), F32)
            slabs = [field[i, pl.ds(width * a, width), :] for a in range(P_SIZE)]
            for a in range(P_SIZE):
                far[3 * f + i, pl.ds(width * a, width), :] = sum(
                    float(table[a, b]) * slabs[b] for b in range(P_SIZE)
                )


def near_derivatives(fields, head, tail):
    high, low = split(fields)

    def apply(table, begin, end):
        return (
            jnp.dot(table[0], high[begin:end], preferred_element_type=F32)
            + jnp.dot(table[1], high[begin:end], preferred_element_type=F32)
            + jnp.dot(table[0], low[begin:end], preferred_element_type=F32)
        )

    upper = apply(head, 0, 256)
    lower = apply(tail, BACK, NODES)
    return [
        jnp.concatenate([upper[j * HEAD : (j + 1) * HEAD], lower[j * TAIL : (j + 1) * TAIL]], axis=0)
        for j in range(2)
    ]


def element_terms(far, near, spacing, live, contract):
    slots = spacing.shape[1]

    def grad(field, i, j):
        column = (3 * field + i) * slots
        return near[j - 1][:, column : column + slots] if j else far[3 * field + i]

    def product(c, j):
        return sum(grad(0, i, c) * grad(1, i, j) for i in range(3))

    pairs = [(0, 1), (0, 2), (1, 2)]
    stack = [product(m, m) for m in range(3)]
    stack += [product(c, j) + product(j, c) for c, j in pairs]
    stack += [sum(grad(0, i, j) * grad(0, i, j) for i in range(3)) for j in range(3)]
    stack_high, stack_low = split(jnp.concatenate(stack, axis=1))
    both = jnp.dot(contract, stack_high, preferred_element_type=F32)
    sums = both[:32] + both[32:] + jnp.dot(contract[:32], stack_low, preferred_element_type=F32)

    def part(j, column):
        return sums[8 * j : 8 * j + 8, column * slots : (column + 1) * slots]

    factor = [2.0 / spacing[j : j + 1] for j in range(3)]
    square = [f * f for f in factor]
    jacobian = spacing[0:1] * spacing[1:2] * spacing[2:3] * 0.125
    terms = []
    for c in range(3):
        total = sum(square[m] * part(c, m) for m in range(3)) - 2.0 * square[c] * part(c, c)
        for column, pair in enumerate(pairs):
            if c in pair:
                j = pair[0] + pair[1] - c
                total = total - square[j] * part(j, 3 + column)
        terms.append(jnp.where(live, total * (factor[c] * jacobian), 0.0))
    spent = sum(square[j] * part(3, 6 + j) for j in range(3)) * jacobian
    return (terms, jnp.where(live, spent, 0.0))


def place(index, rows, values=None):
    slots = index.shape[1]
    row = lax.broadcasted_iota(jnp.int32, (rows, slots), 0)
    columns = []
    for k in range(8):
        hit = row == index[k : k + 1]
        if values is None:
            columns.append(jnp.where(hit, 1.0, 0.0).astype(BF16))
        else:
            columns.append(
                jnp.concatenate(
                    [jnp.where(hit, v[k : k + 1], 0.0).astype(BF16) for v in values], axis=0
                )
            )
    return jnp.concatenate(columns, axis=1)


def far_first(groups, grp):
    place = jnp.minimum(grp, groups - 1 - grp)
    sign = 1 - 2 * (2 * grp // groups)
    single = groups - 1 - 2 * place
    steps = []
    for turn in range(groups - 1):
        rest = turn - single
        pair = (place - rest // 2) * (1 - 2 * lax.rem(rest + 2 * groups, 2))
        offset = jnp.where(rest < 0, groups - 1 - place - turn, pair)
        steps.append(lax.rem(sign * offset + groups, groups))
    return steps


def kernel(
    groups, columns,
    velocity_in, adjoint_in, spacing_in, count_in, map_in, head_in, tail_in, contract_in,
    direction, objective,
    velocity, adjoint, spacing, count, design_map, head, tail, contract, far,
    outgoing, arrived, gathered,
    local_sem, send_sem, recv_sem, hand_sem, send_all, recv_all,
):
    devices = groups * columns
    grp, col = lax.axis_index("grp"), lax.axis_index("elem")
    me = grp * columns + col
    slots = spacing.shape[1]

    barrier = pltpu.get_barrier_semaphore()
    pairs = [
        (velocity_in, velocity), (adjoint_in, adjoint), (head_in, head), (tail_in, tail),
        (map_in, design_map), (spacing_in, spacing), (count_in, count), (contract_in, contract),
    ]
    loads = [pltpu.make_async_copy(a, b, local_sem.at[i]) for i, (a, b) in enumerate(pairs)]
    for load in loads:
        load.start()

    steps = far_first(groups, grp)

    def at(step, turn):
        return (lax.rem(grp + step, groups), lax.rem(col + turn, columns))

    everyone = [(step, turn) for step in steps for turn in range(columns)]
    everyone += [(0, turn) for turn in range(1, columns)]
    for step, turn in everyone:
        pl.semaphore_signal(barrier, inc=1, device_id=at(step, turn), device_id_type=MESH)
    for load in loads[:4]:
        load.wait()

    fields = jnp.concatenate([f[i] for f in (velocity, adjoint) for i in range(3)], axis=1)
    near = near_derivatives(fields, head, tail)
    far_derivatives(velocity, adjoint, far)

    for load in loads[4:]:
        load.wait()
    odd = lax.rem(col, 2)
    partner = col + 1 - 2 * odd
    outer = lax.rem(col + 2 * odd + columns - 1, columns)

    def message(slot, there):
        return pltpu.make_async_remote_copy(
            src_ref=outgoing,
            dst_ref=arrived.at[slot],
            send_sem=send_sem,
            recv_sem=recv_sem.at[slot],
            device_id=there,
            device_id_type=MESH,
        )

    def hand_on(slot):
        return pltpu.make_async_remote_copy(
            src_ref=arrived.at[slot],
            dst_ref=arrived.at[slot],
            send_sem=hand_sem,
            recv_sem=recv_sem.at[slot],
            device_id=(grp, partner),
            device_id_type=MESH,
        )

    def whole(ref, count, semaphore):
        part = ref.at[pl.ds(0, count)]
        return pltpu.make_async_remote_copy(
            src_ref=part,
            dst_ref=part,
            send_sem=semaphore,
            recv_sem=semaphore,
            device_id=(grp, partner),
            device_id_type=MESH,
        )

    def along(parity, step):
        return groups + parity * (groups - 1) + step

    messages = []
    for step in steps:
        there = lax.rem(grp + step, groups)
        messages.append(message(along(odd, step), (there, col + 1 - odd)))
        messages.append(message(1 + step, (there, outer)))
    messages.append(message(1, (grp, outer)))
    messages.append(message(0, (grp, partner)))

    live = lax.broadcasted_iota(jnp.int32, (8, slots), 1) < count[0]
    terms, spent = element_terms(far, near, spacing[...], live, contract[...])
    for c in range(3):
        outgoing[8 * c : 8 * c + 8, :] = terms[c]
    outgoing[24:32, :] = design_map[...].astype(F32)
    pl.semaphore_wait(barrier, devices - 1)
    for copy in messages:
        copy.start()

    base = me * UPPER

    def collect(block):
        nodes = block[24:32].astype(jnp.int32)
        term = block[:24]
        lower = place(nodes & (LANES - 1), LANES)
        index = lax.shift_right_logical(nodes, jnp.full_like(nodes, LANES.bit_length() - 1)) - base
        highs = [term[8 * c : 8 * c + 8].astype(BF16).astype(F32) for c in range(3)]
        lows = [term[8 * c : 8 * c + 8] - highs[c] for c in range(3)]
        return lax.dot_general(
            place(index, UPPER, highs + lows),
            lower,
            (((1,), (1,)), ((), ())),
            preferred_element_type=F32,
        )

    both = collect(outgoing[...])
    order = [(0, False), (1, False)]
    for step in steps[::-1]:
        order += [(along(0, step), True), (along(1, step), True), (1 + step, False)]
    for slot, shared in order:
        hand_on(slot).wait_recv()
        if shared:

            @pl.when(odd == 1)
            def _():
                hand_on(slot).start()

        both = both + collect(arrived[slot])
    total = both[: 3 * UPPER] + both[3 * UPPER :]

    squares = total * total
    squares = sum(squares[8 * i : 8 * i + 8] for i in range(3 * UPPER // 8))
    lane = lax.broadcasted_iota(jnp.int32, (8, LANES), 1)
    mixed = jnp.where(
        lane < LANES // 2,
        squares + pltpu.roll(squares, LANES // 2, 1),
        spent + pltpu.roll(spent, LANES // 2, 1),
    )
    gathered[devices - 1] = jnp.sum(mixed, axis=0, keepdims=True)

    def share(step, turn):
        slot = step * columns + turn - 1
        return pltpu.make_async_remote_copy(
            src_ref=gathered.at[devices - 1],
            dst_ref=gathered.at[slot],
            send_sem=send_all,
            recv_sem=recv_all,
            device_id=at(step, turn),
            device_id_type=MESH,
        )

    for step, turn in everyone:
        share(step, turn).start()
    whole(arrived, len(messages), send_sem).wait_send()
    whole(gathered, devices - 1, recv_all).wait_recv()
    everything = jnp.sum(gathered[...], axis=0)
    first = lax.broadcasted_iota(jnp.int32, (1, LANES), 1) < LANES // 2
    square_total = jnp.sum(jnp.where(first, everything, 0.0), axis=1, keepdims=True)
    spent_total = jnp.sum(jnp.where(first, 0.0, everything), axis=1, keepdims=True)
    scale = lax.rsqrt(square_total * (1.0 / (3.0 * ND_DEV * devices)) + 1e-06)
    scaled = total * scale
    for c in range(3):
        direction[c] = scaled[UPPER * c : UPPER * c + UPPER]
    objective[...] = jnp.broadcast_to(spent_total * (1.0 / (NODES * slots * devices)), (1, LANES))
    whole(gathered, devices - 1, send_all).wait_send()

    @pl.when(odd == 1)
    def _():
        whole(arrived, 2 * (groups - 1), hand_sem).wait_send()


def hand_over(scaled, spent, direction, objective):
    for c in range(3):
        for u in range(UPPER):
            direction[c : c + 1, u * LANES : (u + 1) * LANES] = scaled[c, u : u + 1, :]
    objective[...] = spent[:, :1]


def body(groups, columns, velocity, adjoint, spacing, elem_count, design_map):
    devices = groups * columns
    blocks = 3 * groups
    slots = spacing.shape[1]
    vmem = pl.BlockSpec(memory_space=pltpu.VMEM)
    constants = tables()
    operands = [
        pltpu.with_memory_space_constraint(jnp.asarray(x), pltpu.HBM)
        for x in (velocity, adjoint, spacing)
    ]
    operands.append(elem_count)
    operands += [
        pltpu.with_memory_space_constraint(jnp.asarray(x), pltpu.HBM)
        for x in (design_map, *constants)
    ]
    scaled, spent = pl.pallas_call(
        functools.partial(kernel, groups, columns),
        out_shape=(
            jax.ShapeDtypeStruct((3, UPPER, LANES), F32),
            jax.ShapeDtypeStruct((1, LANES), F32),
        ),
        in_specs=[pl.BlockSpec(memory_space=pltpu.HBM)] * 8,
        out_specs=(vmem, vmem),
        scratch_shapes=[
            pltpu.VMEM(velocity.shape, F32),
            pltpu.VMEM(adjoint.shape, F32),
            pltpu.VMEM(spacing.shape, F32),
            pltpu.SMEM((1,), jnp.int32),
            pltpu.VMEM((8, slots), jnp.int32),
            *[pltpu.VMEM(table.shape, BF16) for table in constants],
            pltpu.VMEM((6, ROWS, slots), F32),
            pltpu.VMEM((32, slots), F32),
            pltpu.VMEM((blocks - 1, 32, slots), F32),
            pltpu.VMEM((devices, 1, LANES), F32),
            pltpu.SemaphoreType.DMA((8,)),
            pltpu.SemaphoreType.DMA,
            pltpu.SemaphoreType.DMA((blocks - 1,)),
            *[pltpu.SemaphoreType.DMA] * 3,
        ],
        compiler_params=pltpu.CompilerParams(
            collective_id=0, has_side_effects=True, vmem_limit_bytes=VMEM_BYTES
        ),
    )(*operands)
    direction, objective = pl.pallas_call(
        hand_over,
        out_shape=(
            jax.ShapeDtypeStruct((3, ND_DEV), F32),
            jax.ShapeDtypeStruct((1, 1), F32),
        ),
        in_specs=[vmem] * 2,
        out_specs=(vmem, vmem),
        compiler_params=pltpu.CompilerParams(vmem_limit_bytes=VMEM_BYTES),
    )(scaled, spent)
    return (direction, objective.reshape(()))


def solution(mesh):
    return jax.shard_map(
        functools.partial(body, mesh.shape["grp"], mesh.shape["elem"]),
        mesh=mesh,
        in_specs=(
            P(None, None, ("grp", "elem")),
            P(None, None, ("grp", "elem")),
            P(None, ("grp", "elem")),
            P(("grp", "elem")),
            P(None, ("grp", "elem")),
        ),
        out_specs=(P(None, ("grp", "elem")), P()),
        check_vma=False,
    )
```

```python
import functools

import jax
import jax.numpy as jnp
import numpy as np
from jax import lax
from jax.experimental import pallas as pl
from jax.experimental.pallas import tpu as pltpu
from jax.sharding import PartitionSpec as P

P_SIZE = 7
ND_DEV = 2048
LANES = 128
UPPER = ND_DEV // LANES
NODES = P_SIZE**3
FACE = P_SIZE * P_SIZE
CHUNKS = -(-FACE // 8)
SLAB = 8 * CHUNKS
DEEP = 64
HALF = P_SIZE // 2
MESH = pl.DeviceIdType.MESH
F32 = jnp.float32
BF16 = jnp.bfloat16
VMEM_BYTES = 32 * 2**20


def lobatto(degree):
    points = np.cos(np.pi * np.arange(degree + 1) / degree)
    for sweep in range(60):
        lower = np.ones(degree + 1)
        upper = points.copy()
        for order in range(2, degree + 1):
            lower, upper = (upper, ((2 * order - 1) * points * upper - (order - 1) * lower) / order)
        points = points - (points * upper - lower) / ((degree + 1) * upper)
    lower = np.ones(degree + 1)
    upper = points.copy()
    for order in range(2, degree + 1):
        lower, upper = (upper, ((2 * order - 1) * points * upper - (order - 1) * lower) / order)
    return (points[::-1].copy(), upper[::-1].copy())


def halves(table):
    exact = np.asarray(table, np.float32)
    high = exact.astype(BF16)
    low = (exact - high.astype(np.float32)).astype(BF16)
    return (high, low)


def derivative_table():
    degree = P_SIZE - 1
    points, values = lobatto(degree)
    derivative = np.zeros((P_SIZE, P_SIZE))
    for i in range(P_SIZE):
        for j in range(P_SIZE):
            if i != j:
                derivative[i, j] = values[i] / (values[j] * (points[i] - points[j]))
    derivative[0, 0] = -degree * (degree + 1) / 4.0
    derivative[P_SIZE - 1, P_SIZE - 1] = degree * (degree + 1) / 4.0
    return derivative


def triple(table, rows):
    wide = np.zeros((rows, DEEP))
    wide[: table.shape[0], :FACE] = table
    high, low = halves(wide)
    return np.concatenate([high, high, low], axis=1)


def quadrature():
    degree = P_SIZE - 1
    points, values = lobatto(degree)
    return (points, 2.0 / (degree * (degree + 1) * values**2))


def tables():
    points, weights = quadrature()
    derivative = derivative_table()
    unit = np.eye(P_SIZE)
    near = [triple(t, SLAB) for t in (np.kron(derivative, unit), np.kron(unit, derivative))]
    coords = [c.reshape(-1) for c in np.meshgrid(points, points, indexing="ij")]
    face = np.outer(weights, weights).reshape(-1)
    even = np.zeros((24, FACE))
    uneven = np.zeros((24, FACE))
    for vertex in range(8):
        signs = [2.0 * (vertex >> 2 - m & 1) - 1.0 for m in range(3)]
        first, second = [(1.0 + signs[m + 1] * coords[m]) / 2.0 for m in range(2)]
        even[vertex] = signs[0] / 2.0 * first * second * face
        even[8 + vertex] = signs[1] / 4.0 * second * face
        even[16 + vertex] = signs[2] / 4.0 * first * face
        uneven[8 + vertex] = signs[0] * even[8 + vertex]
        uneven[16 + vertex] = signs[0] * even[16 + vertex]
    weigh = np.zeros((SLAB, LANES), np.float32)
    weigh[:FACE] = face[:, None]
    return (
        np.concatenate(near, axis=0),
        np.concatenate([triple(even, 32), triple(uneven, 32)], axis=1),
        weigh,
    )


def split(value):
    high = value.astype(BF16)
    return (high, (value - high.astype(F32)).astype(BF16))


def chunk(field, i, a, r):
    start = FACE * a + 8 * r
    if start + 8 <= NODES:
        return field[i, pl.ds(start, 8), :]
    rest = NODES - start
    row = lax.broadcasted_iota(jnp.int32, (8, field.shape[2]), 0)
    value = jnp.zeros((8, field.shape[2]), F32)
    for k in range(rest):
        value = jnp.where(row == k, field[i, pl.ds(start + k, 1), :], value)
    return value


def stacked(parts):
    high, low = split(jnp.concatenate(parts, axis=0))
    return jnp.concatenate([high, low, high], axis=0)


def near_derivatives(velocity, adjoint, table, near):
    blank = jnp.zeros((DEEP - SLAB, velocity.shape[2]), F32)
    for a in range(P_SIZE):
        fields = [
            stacked([*[chunk(field, i, a, r) for r in range(CHUNKS)], blank])
            for field in (velocity, adjoint)
            for i in range(3)
        ]
        near[a] = jnp.dot(
            table[...], jnp.concatenate(fields, axis=1), preferred_element_type=F32
        )


def far_derivatives(velocity, adjoint, far):
    table = derivative_table()
    for f in range(6):
        field = (velocity, adjoint)[f // 3]
        for r in range(CHUNKS):
            x = [chunk(field, f % 3, a, r) for a in range(P_SIZE)]
            plus = [x[j] + x[P_SIZE - 1 - j] for j in range(HALF)]
            minus = [x[j] - x[P_SIZE - 1 - j] for j in range(HALF)]

            def put(a, value):
                far[f, a, 8 * r : 8 * r + 8, :] = value

            for i in range(HALF):
                mirror = table[i, ::-1]
                even = float(table[i, HALF]) * x[HALF] + sum(
                    float(table[i, j] + mirror[j]) / 2.0 * plus[j] for j in range(HALF)
                )
                uneven = sum(float(table[i, j] - mirror[j]) / 2.0 * minus[j] for j in range(HALF))
                put(i, uneven + even)
                put(P_SIZE - 1 - i, uneven - even)
            put(HALF, sum(float(table[HALF, j]) * minus[j] for j in range(HALF)))


PAIRS = [(0, 1), (0, 2), (1, 2)]


def reduced(far, near, r, slots):
    points, weights = quadrature()

    def products(a):
        def grad(f, j):
            if j == 0:
                return far[f, a, 8 * r : 8 * r + 8, :]
            row = SLAB * (j - 1) + 8 * r
            return near[a, row : row + 8, f * slots : (f + 1) * slots]

        u = [[grad(i, j) for j in range(3)] for i in range(3)]
        w = [[grad(3 + i, j) for j in range(3)] for i in range(3)]
        stress = [sum(u[i][m] * w[i][m] for i in range(3)) for m in range(3)]
        stress += [
            sum(u[i][c] * w[i][j] for i in range(3)) + sum(w[i][c] * u[i][j] for i in range(3))
            for c, j in PAIRS
        ]
        return (stress, [sum(u[i][j] * u[i][j] for i in range(3)) for j in range(3)])

    stress, spent = products(HALF)
    even = [float(weights[HALF]) * s for s in stress]
    spent = [float(weights[HALF]) * s for s in spent]
    uneven = [None] * 6
    for a in range(HALF):
        here, here_spent = products(a)
        there, there_spent = products(P_SIZE - 1 - a)
        weight, moment = float(weights[a]), float(weights[a] * points[a])
        for k in range(6):
            even[k] = even[k] + weight * (here[k] + there[k])
            part = moment * (here[k] - there[k])
            uneven[k] = part if a == 0 else uneven[k] + part
        for k in range(3):
            spent[k] = spent[k] + weight * (here_spent[k] + there_spent[k])
    return (even, uneven, spent)


def element_terms(far, near, spacing, live, contract, weigh):
    slots = spacing.shape[1]
    factor = [2.0 / spacing[j : j + 1] for j in range(3)]
    square = [f * f for f in factor]
    jacobian = spacing[0:1] * spacing[1:2] * spacing[2:3] * 0.125
    rows = [reduced(far, near, r, slots) for r in range(CHUNKS)]
    lost = 0.0
    for r in range(CHUNKS):
        level = sum(square[j] * rows[r][2][j] for j in range(3))
        lost = lost + weigh[8 * r : 8 * r + 8, :slots] * level
    blank = jnp.zeros((DEEP - SLAB, slots), F32)
    columns = [
        jnp.concatenate([stacked([*[row[p][k] for row in rows], blank]) for p in range(2)], axis=0)
        for k in range(6)
    ]
    sums = jnp.dot(contract, jnp.concatenate(columns, axis=1), preferred_element_type=F32)

    def part(j, column):
        return sums[8 * j : 8 * j + 8, column * slots : (column + 1) * slots]

    terms = []
    for c in range(3):
        total = sum(square[m] * part(c, m) for m in range(3)) - 2.0 * square[c] * part(c, c)
        for column, pair in enumerate(PAIRS):
            if c in pair:
                j = pair[0] + pair[1] - c
                total = total - square[j] * part(j, 3 + column)
        terms.append(jnp.where(live, total * (factor[c] * jacobian), 0.0))
    return (terms, jnp.where(live, lost * jacobian, 0.0))


def spread(row):
    return jnp.broadcast_to(row, (16, row.shape[1])).astype(BF16)


def place(index, rows, values=None):
    slots = index.shape[1]
    row = lax.broadcasted_iota(jnp.int32, (rows, slots), 0).astype(F32).astype(BF16)
    index = index.astype(F32)
    zero = jnp.zeros((rows, slots), BF16)
    columns = []
    for k in range(8):
        hit = row == jnp.concatenate([spread(index[k : k + 1])] * (rows // 16), axis=0)
        if values is None:
            columns.append(jnp.where(hit, jnp.ones_like(zero), zero))
        else:
            columns.append(
                jnp.concatenate([jnp.where(hit, spread(v[k : k + 1]), zero) for v in values], axis=0)
            )
    return jnp.concatenate(columns, axis=1)


def far_first(groups, grp):
    place = jnp.minimum(grp, groups - 1 - grp)
    sign = 1 - 2 * (2 * grp // groups)
    single = groups - 1 - 2 * place
    steps = []
    for turn in range(groups - 1):
        rest = turn - single
        pair = (place - rest // 2) * (1 - 2 * lax.rem(rest + 2 * groups, 2))
        offset = jnp.where(rest < 0, groups - 1 - place - turn, pair)
        steps.append(lax.rem(sign * offset + groups, groups))
    return steps


def kernel(
    groups, columns,
    velocity_in, adjoint_in, spacing_in, count_in, map_in, table_in, contract_in, weigh_in,
    direction, objective,
    velocity, adjoint, spacing, count, design_map, table, contract, weigh, near, far,
    outgoing, arrived, gathered_sums, gathered,
    local_sem, send_sem, recv_sem, hand_sem, send_all, recv_all,
):
    devices = groups * columns
    grp, col = lax.axis_index("grp"), lax.axis_index("elem")
    me = grp * columns + col
    slots = spacing.shape[1]

    barrier = pltpu.get_barrier_semaphore()
    pairs = [
        (velocity_in, velocity), (adjoint_in, adjoint), (table_in, table),
        (map_in, design_map), (spacing_in, spacing), (count_in, count),
        (contract_in, contract), (weigh_in, weigh),
    ]
    loads = [pltpu.make_async_copy(a, b, local_sem.at[i]) for i, (a, b) in enumerate(pairs)]
    for load in loads:
        load.start()

    steps = far_first(groups, grp)

    def at(step, turn):
        return (lax.rem(grp + step, groups), lax.rem(col + turn, columns))

    everyone = [(step, turn) for step in steps for turn in range(columns)]
    everyone += [(0, turn) for turn in range(1, columns)]
    for step, turn in everyone:
        pl.semaphore_signal(barrier, inc=1, device_id=at(step, turn), device_id_type=MESH)
    for load in loads[:3]:
        load.wait()

    near_derivatives(velocity, adjoint, table, near)
    far_derivatives(velocity, adjoint, far)

    for load in loads[3:]:
        load.wait()
    odd = lax.rem(col, 2)
    partner = col + 1 - 2 * odd
    outer = lax.rem(col + 2 * odd + columns - 1, columns)

    def message(slot, there):
        return pltpu.make_async_remote_copy(
            src_ref=outgoing,
            dst_ref=arrived.at[slot],
            send_sem=send_sem,
            recv_sem=recv_sem.at[slot],
            device_id=there,
            device_id_type=MESH,
        )

    def hand_on(slot):
        return pltpu.make_async_remote_copy(
            src_ref=arrived.at[slot],
            dst_ref=arrived.at[slot],
            send_sem=hand_sem,
            recv_sem=recv_sem.at[slot],
            device_id=(grp, partner),
            device_id_type=MESH,
        )

    def whole(ref, count, semaphore):
        part = ref.at[pl.ds(0, count)]
        return pltpu.make_async_remote_copy(
            src_ref=part,
            dst_ref=part,
            send_sem=semaphore,
            recv_sem=semaphore,
            device_id=(grp, partner),
            device_id_type=MESH,
        )

    def along(parity, step):
        return groups + parity * (groups - 1) + step

    messages = []
    messages.append(message(0, (grp, partner)))
    messages.append(message(1, (grp, outer)))
    for step in steps:
        messages.append(message(along(odd, step), (lax.rem(grp + step, groups), col + 1 - odd)))
    for step in steps:
        messages.append(message(1 + step, (lax.rem(grp + step, groups), outer)))

    live = lax.broadcasted_iota(jnp.int32, (8, slots), 1) < count[0]
    terms, spent = element_terms(far, near, spacing[...], live, contract[...], weigh[...])
    for c in range(3):
        outgoing[8 * c : 8 * c + 8, :] = terms[c]
    outgoing[24:32, :] = design_map[...].astype(F32)
    pl.semaphore_wait(barrier, devices - 1)
    for copy in messages:
        copy.start()

    base = me * UPPER

    def collect(blocks):
        uppers, lowers = [], []
        for block in blocks:
            nodes, term = block[24:32].astype(jnp.int32), block[:24]
            index = lax.shift_right_logical(nodes, jnp.full_like(nodes, LANES.bit_length() - 1)) - base
            highs = [term[8 * c : 8 * c + 8].astype(BF16).astype(F32) for c in range(3)]
            lows = [term[8 * c : 8 * c + 8] - highs[c] for c in range(3)]
            uppers.append(place(index, UPPER, highs + lows))
            lowers.append(place(nodes & (LANES - 1), LANES))
        return lax.dot_general(
            jnp.concatenate(uppers, axis=1),
            jnp.concatenate(lowers, axis=1),
            (((1,), (1,)), ((), ())),
            preferred_element_type=F32,
        )

    def arrive(slot):
        hand_on(slot).wait_recv()

    near_first = steps[::-1]
    shared = [along(parity, step) for step in near_first for parity in range(2)]
    direct = [1 + step for step in [0, *near_first]]

    def add(slots_in):
        gathered_sums[...] += collect([arrived[slot] for slot in slots_in])

    both = collect([outgoing[...]])
    arrive(0)
    gathered_sums[...] = both + collect([arrived[0]])

    @pl.when(odd == 1)
    def _():
        for slot in shared:
            arrive(slot)
            hand_on(slot).start()
        arrive(direct[0])
        add([direct[0], *shared])
        for slot in direct[1:]:
            arrive(slot)
        add(direct[1:])

    @pl.when(odd == 0)
    def _():
        for slot in direct:
            arrive(slot)
        add(direct)
        for slot in shared:
            arrive(slot)
        add(shared)

    both = gathered_sums[...]
    total = both[: 3 * UPPER] + both[3 * UPPER :]

    squares = total * total
    squares = sum(squares[8 * i : 8 * i + 8] for i in range(3 * UPPER // 8))
    lane = lax.broadcasted_iota(jnp.int32, (8, LANES), 1)
    mixed = jnp.where(
        lane < LANES // 2,
        squares + pltpu.roll(squares, LANES // 2, 1),
        spent + pltpu.roll(spent, LANES // 2, 1),
    )
    gathered[devices - 1] = jnp.sum(mixed, axis=0, keepdims=True)

    def share(step, turn):
        slot = step * columns + turn - 1
        return pltpu.make_async_remote_copy(
            src_ref=gathered.at[devices - 1],
            dst_ref=gathered.at[slot],
            send_sem=send_all,
            recv_sem=recv_all,
            device_id=at(step, turn),
            device_id_type=MESH,
        )

    for step, turn in everyone:
        share(step, turn).start()
    whole(arrived, len(messages), send_sem).wait_send()
    whole(gathered, devices - 1, recv_all).wait_recv()
    everything = jnp.sum(gathered[...], axis=0)
    first = lax.broadcasted_iota(jnp.int32, (1, LANES), 1) < LANES // 2
    square_total = jnp.sum(jnp.where(first, everything, 0.0), axis=1, keepdims=True)
    spent_total = jnp.sum(jnp.where(first, 0.0, everything), axis=1, keepdims=True)
    scale = lax.rsqrt(square_total * (1.0 / (3.0 * ND_DEV * devices)) + 1e-06)
    scaled = total * scale
    for c in range(3):
        direction[c] = scaled[UPPER * c : UPPER * c + UPPER]
    objective[...] = jnp.broadcast_to(spent_total * (1.0 / (NODES * slots * devices)), (1, LANES))
    whole(gathered, devices - 1, send_all).wait_send()

    @pl.when(odd == 1)
    def _():
        whole(arrived, 2 * (groups - 1), hand_sem).wait_send()


def hand_over(scaled, spent, direction, objective):
    for c in range(3):
        for u in range(UPPER):
            direction[c : c + 1, u * LANES : (u + 1) * LANES] = scaled[c, u : u + 1, :]
    objective[...] = spent[:, :1]


def body(groups, columns, velocity, adjoint, spacing, elem_count, design_map):
    devices = groups * columns
    blocks = 3 * groups
    slots = spacing.shape[1]
    vmem = pl.BlockSpec(memory_space=pltpu.VMEM)
    constants = tables()
    operands = [
        pltpu.with_memory_space_constraint(jnp.asarray(x), pltpu.HBM)
        for x in (velocity, adjoint, spacing)
    ]
    operands.append(elem_count)
    operands += [
        pltpu.with_memory_space_constraint(jnp.asarray(x), pltpu.HBM)
        for x in (design_map, *constants)
    ]
    scaled, spent = pl.pallas_call(
        functools.partial(kernel, groups, columns),
        out_shape=(
            jax.ShapeDtypeStruct((3, UPPER, LANES), F32),
            jax.ShapeDtypeStruct((1, LANES), F32),
        ),
        in_specs=[pl.BlockSpec(memory_space=pltpu.HBM)] * 8,
        out_specs=(vmem, vmem),
        scratch_shapes=[
            pltpu.VMEM(velocity.shape, F32),
            pltpu.VMEM(adjoint.shape, F32),
            pltpu.VMEM(spacing.shape, F32),
            pltpu.SMEM((1,), jnp.int32),
            pltpu.VMEM((8, slots), jnp.int32),
            *[pltpu.VMEM(table.shape, table.dtype) for table in constants],
            pltpu.VMEM((P_SIZE, 2 * SLAB, 6 * slots), F32),
            pltpu.VMEM((6, P_SIZE, SLAB, slots), F32),
            pltpu.VMEM((32, slots), F32),
            pltpu.VMEM((blocks - 1, 32, slots), F32),
            pltpu.VMEM((6 * UPPER, LANES), F32),
            pltpu.VMEM((devices, 1, LANES), F32),
            pltpu.SemaphoreType.DMA((8,)),
            pltpu.SemaphoreType.DMA,
            pltpu.SemaphoreType.DMA((blocks - 1,)),
            *[pltpu.SemaphoreType.DMA] * 3,
        ],
        compiler_params=pltpu.CompilerParams(
            collective_id=0, has_side_effects=True, vmem_limit_bytes=VMEM_BYTES
        ),
    )(*operands)
    direction, objective = pl.pallas_call(
        hand_over,
        out_shape=(
            jax.ShapeDtypeStruct((3, ND_DEV), F32),
            jax.ShapeDtypeStruct((1, 1), F32),
        ),
        in_specs=[vmem] * 2,
        out_specs=(vmem, vmem),
        compiler_params=pltpu.CompilerParams(vmem_limit_bytes=VMEM_BYTES),
    )(scaled, spent)
    return (direction, objective.reshape(()))


def solution(mesh):
    return jax.shard_map(
        functools.partial(body, mesh.shape["grp"], mesh.shape["elem"]),
        mesh=mesh,
        in_specs=(
            P(None, None, ("grp", "elem")),
            P(None, None, ("grp", "elem")),
            P(None, ("grp", "elem")),
            P(("grp", "elem")),
            P(None, ("grp", "elem")),
        ),
        out_specs=(P(None, ("grp", "elem")), P()),
        check_vma=False,
    )
```

```python
import functools

import jax
import jax.numpy as jnp
import numpy as np
from jax import lax
from jax.experimental import pallas as pl
from jax.experimental.pallas import tpu as pltpu
from jax.sharding import PartitionSpec as P

P_SIZE = 7
ND_DEV = 2048
LANES = 128
UPPER = ND_DEV // LANES
NODES = P_SIZE**3
FACE = P_SIZE * P_SIZE
CHUNKS = -(-FACE // 8)
SLAB = 8 * CHUNKS
DEEP = 64
HALF = P_SIZE // 2
MESH = pl.DeviceIdType.MESH
F32 = jnp.float32
BF16 = jnp.bfloat16
VMEM_BYTES = 32 * 2**20


def lobatto(degree):
    points = np.cos(np.pi * np.arange(degree + 1) / degree)
    for sweep in range(60):
        lower = np.ones(degree + 1)
        upper = points.copy()
        for order in range(2, degree + 1):
            lower, upper = (upper, ((2 * order - 1) * points * upper - (order - 1) * lower) / order)
        points = points - (points * upper - lower) / ((degree + 1) * upper)
    lower = np.ones(degree + 1)
    upper = points.copy()
    for order in range(2, degree + 1):
        lower, upper = (upper, ((2 * order - 1) * points * upper - (order - 1) * lower) / order)
    return (points[::-1].copy(), upper[::-1].copy())


def halves(table):
    exact = np.asarray(table, np.float32)
    high = exact.astype(BF16)
    low = (exact - high.astype(np.float32)).astype(BF16)
    return (high, low)


def derivative_table():
    degree = P_SIZE - 1
    points, values = lobatto(degree)
    derivative = np.zeros((P_SIZE, P_SIZE))
    for i in range(P_SIZE):
        for j in range(P_SIZE):
            if i != j:
                derivative[i, j] = values[i] / (values[j] * (points[i] - points[j]))
    derivative[0, 0] = -degree * (degree + 1) / 4.0
    derivative[P_SIZE - 1, P_SIZE - 1] = degree * (degree + 1) / 4.0
    return derivative


def triple(table, rows):
    wide = np.zeros((rows, DEEP))
    wide[: table.shape[0], :FACE] = table
    high, low = halves(wide)
    return np.concatenate([high, high, low], axis=1)


def quadrature():
    degree = P_SIZE - 1
    points, values = lobatto(degree)
    return (points, 2.0 / (degree * (degree + 1) * values**2))


def tables():
    points, weights = quadrature()
    derivative = derivative_table()
    unit = np.eye(P_SIZE)
    near = [triple(t, SLAB) for t in (np.kron(derivative, unit), np.kron(unit, derivative))]
    coords = [c.reshape(-1) for c in np.meshgrid(points, points, indexing="ij")]
    face = np.outer(weights, weights).reshape(-1)
    even = np.zeros((24, FACE))
    uneven = np.zeros((24, FACE))
    for vertex in range(8):
        signs = [2.0 * (vertex >> 2 - m & 1) - 1.0 for m in range(3)]
        first, second = [(1.0 + signs[m + 1] * coords[m]) / 2.0 for m in range(2)]
        even[vertex] = signs[0] / 2.0 * first * second * face
        even[8 + vertex] = signs[1] / 4.0 * second * face
        even[16 + vertex] = signs[2] / 4.0 * first * face
        uneven[8 + vertex] = signs[0] * even[8 + vertex]
        uneven[16 + vertex] = signs[0] * even[16 + vertex]
    return np.concatenate([*near, triple(even, 32), triple(uneven, 32)], axis=0)


def face_weights(r, slots):
    points, weights = quadrature()
    face = np.outer(weights, weights).reshape(-1)
    row = lax.broadcasted_iota(jnp.int32, (8, slots), 0)
    value = jnp.zeros((8, slots), F32)
    for k, weight in enumerate(face[8 * r : 8 * r + 8]):
        value = jnp.where(row == k, float(weight), value)
    return value


def split(value):
    high = value.astype(BF16)
    return (high, (value - high.astype(F32)).astype(BF16))


def chunk(field, i, a, r):
    start = FACE * a + 8 * r
    if start + 8 <= NODES:
        return field[i, pl.ds(start, 8), :]
    rest = NODES - start
    row = lax.broadcasted_iota(jnp.int32, (8, field.shape[2]), 0)
    value = jnp.zeros((8, field.shape[2]), F32)
    for k in range(rest):
        value = jnp.where(row == k, field[i, pl.ds(start + k, 1), :], value)
    return value


def stacked(parts):
    high, low = split(jnp.concatenate(parts, axis=0))
    return jnp.concatenate([high, low, high], axis=0)


def near_derivatives(velocity, adjoint, table, near):
    blank = jnp.zeros((DEEP - SLAB, velocity.shape[2]), F32)
    for a in range(P_SIZE):
        fields = [
            stacked([*[chunk(field, i, a, r) for r in range(CHUNKS)], blank])
            for field in (velocity, adjoint)
            for i in range(3)
        ]
        near[a] = jnp.dot(
            table[: 2 * SLAB], jnp.concatenate(fields, axis=1), preferred_element_type=F32
        )


def far_derivatives(velocity, adjoint, far):
    table = derivative_table()
    for f in range(6):
        field = (velocity, adjoint)[f // 3]
        for r in range(CHUNKS):
            x = [chunk(field, f % 3, a, r) for a in range(P_SIZE)]
            plus = [x[j] + x[P_SIZE - 1 - j] for j in range(HALF)]
            minus = [x[j] - x[P_SIZE - 1 - j] for j in range(HALF)]

            def put(a, value):
                far[f, a, 8 * r : 8 * r + 8, :] = value

            for i in range(HALF):
                mirror = table[i, ::-1]
                even = float(table[i, HALF]) * x[HALF] + sum(
                    float(table[i, j] + mirror[j]) / 2.0 * plus[j] for j in range(HALF)
                )
                uneven = sum(float(table[i, j] - mirror[j]) / 2.0 * minus[j] for j in range(HALF))
                put(i, uneven + even)
                put(P_SIZE - 1 - i, uneven - even)
            put(HALF, sum(float(table[HALF, j]) * minus[j] for j in range(HALF)))


PAIRS = [(0, 1), (0, 2), (1, 2)]


def reduced(far, near, r, slots):
    points, weights = quadrature()

    def products(a):
        def grad(f, j):
            if j == 0:
                return far[f, a, 8 * r : 8 * r + 8, :]
            row = SLAB * (j - 1) + 8 * r
            return near[a, row : row + 8, f * slots : (f + 1) * slots]

        u = [[grad(i, j) for j in range(3)] for i in range(3)]
        w = [[grad(3 + i, j) for j in range(3)] for i in range(3)]
        stress = [sum(u[i][m] * w[i][m] for i in range(3)) for m in range(3)]
        stress += [
            sum(u[i][c] * w[i][j] for i in range(3)) + sum(w[i][c] * u[i][j] for i in range(3))
            for c, j in PAIRS
        ]
        return (stress, [sum(u[i][j] * u[i][j] for i in range(3)) for j in range(3)])

    stress, spent = products(HALF)
    even = [float(weights[HALF]) * s for s in stress]
    spent = [float(weights[HALF]) * s for s in spent]
    uneven = [None] * 6
    for a in range(HALF):
        here, here_spent = products(a)
        there, there_spent = products(P_SIZE - 1 - a)
        weight, moment = float(weights[a]), float(weights[a] * points[a])
        for k in range(6):
            even[k] = even[k] + weight * (here[k] + there[k])
            part = moment * (here[k] - there[k])
            uneven[k] = part if a == 0 else uneven[k] + part
        for k in range(3):
            spent[k] = spent[k] + weight * (here_spent[k] + there_spent[k])
    return (even, uneven, spent)


def element_terms(far, near, spacing, live, table):
    slots = spacing.shape[1]
    factor = [2.0 / spacing[j : j + 1] for j in range(3)]
    square = [f * f for f in factor]
    jacobian = spacing[0:1] * spacing[1:2] * spacing[2:3] * 0.125
    rows = [reduced(far, near, r, slots) for r in range(CHUNKS)]
    lost = 0.0
    for r in range(CHUNKS):
        level = sum(square[j] * rows[r][2][j] for j in range(3))
        lost = lost + face_weights(r, slots) * level
    blank = jnp.zeros((DEEP - SLAB, slots), F32)
    sums = 0.0
    for p in range(2):
        columns = [stacked([*[row[p][k] for row in rows], blank]) for k in range(6)]
        begin = 2 * SLAB + 32 * p
        sums = sums + jnp.dot(
            table[begin : begin + 32],
            jnp.concatenate(columns, axis=1),
            preferred_element_type=F32,
        )

    def part(j, column):
        return sums[8 * j : 8 * j + 8, column * slots : (column + 1) * slots]

    terms = []
    for c in range(3):
        total = sum(square[m] * part(c, m) for m in range(3)) - 2.0 * square[c] * part(c, c)
        for column, pair in enumerate(PAIRS):
            if c in pair:
                j = pair[0] + pair[1] - c
                total = total - square[j] * part(j, 3 + column)
        terms.append(jnp.where(live, total * (factor[c] * jacobian), 0.0))
    return (terms, jnp.where(live, lost * jacobian, 0.0))


def spread(row):
    return jnp.broadcast_to(row, (16, row.shape[1])).astype(BF16)


def place(index, rows, values=None):
    slots = index.shape[1]
    row = lax.broadcasted_iota(jnp.int32, (rows, slots), 0).astype(F32).astype(BF16)
    index = index.astype(F32)
    zero = jnp.zeros((rows, slots), BF16)
    columns = []
    for k in range(8):
        hit = row == jnp.concatenate([spread(index[k : k + 1])] * (rows // 16), axis=0)
        if values is None:
            columns.append(jnp.where(hit, jnp.ones_like(zero), zero))
        else:
            columns.append(
                jnp.concatenate([jnp.where(hit, spread(v[k : k + 1]), zero) for v in values], axis=0)
            )
    return jnp.concatenate(columns, axis=1)


def far_first(groups, grp):
    place = jnp.minimum(grp, groups - 1 - grp)
    sign = 1 - 2 * (2 * grp // groups)
    single = groups - 1 - 2 * place
    steps = []
    for turn in range(groups - 1):
        rest = turn - single
        pair = (place - rest // 2) * (1 - 2 * lax.rem(rest + 2 * groups, 2))
        offset = jnp.where(rest < 0, groups - 1 - place - turn, pair)
        steps.append(lax.rem(sign * offset + groups, groups))
    return steps


def kernel(
    groups, columns,
    velocity_in, adjoint_in, spacing_in, count_in, map_in, table_in,
    direction, objective,
    velocity, adjoint, spacing, count, design_map, table, near, far,
    outgoing, arrived, gathered_sums, gathered,
    local_sem, send_sem, recv_sem, hand_sem, send_all, recv_all,
):
    devices = groups * columns
    grp, col = lax.axis_index("grp"), lax.axis_index("elem")
    me = grp * columns + col
    slots = spacing.shape[1]

    barrier = pltpu.get_barrier_semaphore()
    pairs = [
        (velocity_in, velocity), (adjoint_in, adjoint), (table_in, table),
        (map_in, design_map), (spacing_in, spacing), (count_in, count),
    ]
    loads = [pltpu.make_async_copy(a, b, local_sem.at[i]) for i, (a, b) in enumerate(pairs)]
    for load in loads:
        load.start()

    steps = far_first(groups, grp)

    def at(step, turn):
        return (lax.rem(grp + step, groups), lax.rem(col + turn, columns))

    everyone = [(step, turn) for step in steps for turn in range(columns)]
    everyone += [(0, turn) for turn in range(1, columns)]
    for step, turn in everyone:
        pl.semaphore_signal(barrier, inc=1, device_id=at(step, turn), device_id_type=MESH)
    for load in loads[:3]:
        load.wait()

    near_derivatives(velocity, adjoint, table, near)
    far_derivatives(velocity, adjoint, far)

    for load in loads[3:]:
        load.wait()
    odd = lax.rem(col, 2)
    partner = col + 1 - 2 * odd
    outer = lax.rem(col + 2 * odd + columns - 1, columns)

    def message(slot, there, wait):
        return pltpu.make_async_remote_copy(
            src_ref=outgoing,
            dst_ref=arrived.at[slot],
            send_sem=send_sem,
            recv_sem=recv_sem.at[wait],
            device_id=there,
            device_id_type=MESH,
        )

    def arriving(slot, count, wait):
        part = arrived.at[pl.ds(slot, count)]
        return pltpu.make_async_remote_copy(
            src_ref=part,
            dst_ref=part,
            send_sem=hand_sem,
            recv_sem=recv_sem.at[wait],
            device_id=(grp, partner),
            device_id_type=MESH,
        )

    def pair(step):
        return arriving(along(0, step), 2, 2 + step)

    def whole(ref, count, semaphore):
        part = ref.at[pl.ds(0, count)]
        return pltpu.make_async_remote_copy(
            src_ref=part,
            dst_ref=part,
            send_sem=semaphore,
            recv_sem=semaphore,
            device_id=(grp, partner),
            device_id_type=MESH,
        )

    def along(parity, step):
        return groups + 2 * step - 1 + parity

    messages = []
    messages.append(message(0, (grp, partner), 0))
    messages.append(message(1, (grp, outer), 1))
    for step in steps:
        there = lax.rem(grp + step, groups)
        messages.append(message(along(odd, step), (there, col + 1 - odd), 2 + step))
        messages.append(message(1 + step, (there, outer), 2))

    live = lax.broadcasted_iota(jnp.int32, (8, slots), 1) < count[0]
    terms, spent = element_terms(far, near, spacing[...], live, table)
    for c in range(3):
        outgoing[8 * c : 8 * c + 8, :] = terms[c]
    outgoing[24:32, :] = design_map[...].astype(F32)
    pl.semaphore_wait(barrier, devices - 1)
    for copy in messages:
        copy.start()

    base = me * UPPER

    def collect(blocks):
        uppers, lowers = [], []
        for block in blocks:
            nodes, term = block[24:32].astype(jnp.int32), block[:24]
            index = lax.shift_right_logical(nodes, jnp.full_like(nodes, LANES.bit_length() - 1)) - base
            highs = [term[8 * c : 8 * c + 8].astype(BF16).astype(F32) for c in range(3)]
            lows = [term[8 * c : 8 * c + 8] - highs[c] for c in range(3)]
            uppers.append(place(index, UPPER, highs + lows))
            lowers.append(place(nodes & (LANES - 1), LANES))
        return lax.dot_general(
            jnp.concatenate(uppers, axis=1),
            jnp.concatenate(lowers, axis=1),
            (((1,), (1,)), ((), ())),
            preferred_element_type=F32,
        )

    near_first = steps[::-1]
    shared = [along(parity, step) for step in near_first for parity in range(2)]
    direct = [1 + step for step in range(1, groups)]

    def add(slots_in):
        gathered_sums[...] += collect([arrived[slot] for slot in slots_in])

    both = collect([outgoing[...]])
    arriving(0, 1, 0).wait_recv()
    gathered_sums[...] = both + collect([arrived[0]])

    @pl.when(odd == 1)
    def _():
        for step in near_first:
            pair(step).wait_recv()
            pair(step).start()
        arriving(1, 1, 1).wait_recv()
        add([1, *shared])
        arriving(2, groups - 1, 2).wait_recv()
        add(direct)

    @pl.when(odd == 0)
    def _():
        arriving(1, 1, 1).wait_recv()
        add([1])
        arriving(2, groups - 1, 2).wait_recv()
        add(direct)
        for step in near_first:
            pair(step).wait_recv()
        add(shared)

    both = gathered_sums[...]
    total = both[: 3 * UPPER] + both[3 * UPPER :]

    squares = total * total
    squares = sum(squares[8 * i : 8 * i + 8] for i in range(3 * UPPER // 8))
    lane = lax.broadcasted_iota(jnp.int32, (8, LANES), 1)
    mixed = jnp.where(
        lane < LANES // 2,
        squares + pltpu.roll(squares, LANES // 2, 1),
        spent + pltpu.roll(spent, LANES // 2, 1),
    )
    gathered[devices - 1] = jnp.sum(mixed, axis=0, keepdims=True)

    def share(step, turn):
        slot = step * columns + turn - 1
        return pltpu.make_async_remote_copy(
            src_ref=gathered.at[devices - 1],
            dst_ref=gathered.at[slot],
            send_sem=send_all,
            recv_sem=recv_all,
            device_id=at(step, turn),
            device_id_type=MESH,
        )

    for step, turn in everyone:
        share(step, turn).start()
    whole(arrived, len(messages), send_sem).wait_send()
    whole(gathered, devices - 1, recv_all).wait_recv()
    everything = jnp.sum(gathered[...], axis=0)
    first = lax.broadcasted_iota(jnp.int32, (1, LANES), 1) < LANES // 2
    square_total = jnp.sum(jnp.where(first, everything, 0.0), axis=1, keepdims=True)
    spent_total = jnp.sum(jnp.where(first, 0.0, everything), axis=1, keepdims=True)
    scale = lax.rsqrt(square_total * (1.0 / (3.0 * ND_DEV * devices)) + 1e-06)
    scaled = total * scale
    for c in range(3):
        direction[c] = scaled[UPPER * c : UPPER * c + UPPER]
    objective[...] = jnp.broadcast_to(spent_total * (1.0 / (NODES * slots * devices)), (1, LANES))
    whole(gathered, devices - 1, send_all).wait_send()

    @pl.when(odd == 1)
    def _():
        whole(arrived, 2 * (groups - 1), hand_sem).wait_send()


def hand_over(scaled, spent, direction, objective):
    for c in range(3):
        for u in range(UPPER):
            direction[c : c + 1, u * LANES : (u + 1) * LANES] = scaled[c, u : u + 1, :]
    objective[...] = spent[:, :1]


def body(groups, columns, velocity, adjoint, spacing, elem_count, design_map):
    devices = groups * columns
    blocks = 3 * groups
    slots = spacing.shape[1]
    vmem = pl.BlockSpec(memory_space=pltpu.VMEM)
    constant = tables()
    operands = [
        pltpu.with_memory_space_constraint(jnp.asarray(x), pltpu.HBM)
        for x in (velocity, adjoint, spacing)
    ]
    operands.append(elem_count)
    operands += [
        pltpu.with_memory_space_constraint(jnp.asarray(x), pltpu.HBM)
        for x in (design_map, constant)
    ]
    scaled, spent = pl.pallas_call(
        functools.partial(kernel, groups, columns),
        out_shape=(
            jax.ShapeDtypeStruct((3, UPPER, LANES), F32),
            jax.ShapeDtypeStruct((1, LANES), F32),
        ),
        in_specs=[pl.BlockSpec(memory_space=pltpu.HBM)] * 6,
        out_specs=(vmem, vmem),
        scratch_shapes=[
            pltpu.VMEM(velocity.shape, F32),
            pltpu.VMEM(adjoint.shape, F32),
            pltpu.VMEM(spacing.shape, F32),
            pltpu.SMEM((1,), jnp.int32),
            pltpu.VMEM((8, slots), jnp.int32),
            pltpu.VMEM(constant.shape, BF16),
            pltpu.VMEM((P_SIZE, 2 * SLAB, 6 * slots), F32),
            pltpu.VMEM((6, P_SIZE, SLAB, slots), F32),
            pltpu.VMEM((32, slots), F32),
            pltpu.VMEM((blocks - 1, 32, slots), F32),
            pltpu.VMEM((6 * UPPER, LANES), F32),
            pltpu.VMEM((devices, 1, LANES), F32),
            pltpu.SemaphoreType.DMA((6,)),
            pltpu.SemaphoreType.DMA,
            pltpu.SemaphoreType.DMA((groups + 2,)),
            *[pltpu.SemaphoreType.DMA] * 3,
        ],
        compiler_params=pltpu.CompilerParams(
            collective_id=0, has_side_effects=True, vmem_limit_bytes=VMEM_BYTES
        ),
    )(*operands)
    direction, objective = pl.pallas_call(
        hand_over,
        out_shape=(
            jax.ShapeDtypeStruct((3, ND_DEV), F32),
            jax.ShapeDtypeStruct((1, 1), F32),
        ),
        in_specs=[vmem] * 2,
        out_specs=(vmem, vmem),
        compiler_params=pltpu.CompilerParams(vmem_limit_bytes=VMEM_BYTES),
    )(scaled, spent)
    return (direction, objective.reshape(()))


def solution(mesh):
    return jax.shard_map(
        functools.partial(body, mesh.shape["grp"], mesh.shape["elem"]),
        mesh=mesh,
        in_specs=(
            P(None, None, ("grp", "elem")),
            P(None, None, ("grp", "elem")),
            P(None, ("grp", "elem")),
            P(("grp", "elem")),
            P(None, ("grp", "elem")),
        ),
        out_specs=(P(None, ("grp", "elem")), P()),
        check_vma=False,
    )
```

```python
import functools

import jax
import jax.numpy as jnp
import numpy as np
from jax import lax
from jax.experimental import pallas as pl
from jax.experimental.pallas import tpu as pltpu
from jax.sharding import PartitionSpec as P

P_SIZE = 7
ND_DEV = 2048
LANES = 128
UPPER = ND_DEV // LANES
NODES = P_SIZE**3
FACE = P_SIZE * P_SIZE
CHUNKS = -(-FACE // 8)
SLAB = 8 * CHUNKS
DEEP = 64
HALF = P_SIZE // 2
MESH = pl.DeviceIdType.MESH
F32 = jnp.float32
BF16 = jnp.bfloat16
VMEM_BYTES = 32 * 2**20


def lobatto(degree):
    points = np.cos(np.pi * np.arange(degree + 1) / degree)
    for sweep in range(60):
        lower = np.ones(degree + 1)
        upper = points.copy()
        for order in range(2, degree + 1):
            lower, upper = (upper, ((2 * order - 1) * points * upper - (order - 1) * lower) / order)
        points = points - (points * upper - lower) / ((degree + 1) * upper)
    lower = np.ones(degree + 1)
    upper = points.copy()
    for order in range(2, degree + 1):
        lower, upper = (upper, ((2 * order - 1) * points * upper - (order - 1) * lower) / order)
    return (points[::-1].copy(), upper[::-1].copy())


def halves(table):
    exact = np.asarray(table, np.float32)
    high = exact.astype(BF16)
    low = (exact - high.astype(np.float32)).astype(BF16)
    return (high, low)


def derivative_table():
    degree = P_SIZE - 1
    points, values = lobatto(degree)
    derivative = np.zeros((P_SIZE, P_SIZE))
    for i in range(P_SIZE):
        for j in range(P_SIZE):
            if i != j:
                derivative[i, j] = values[i] / (values[j] * (points[i] - points[j]))
    derivative[0, 0] = -degree * (degree + 1) / 4.0
    derivative[P_SIZE - 1, P_SIZE - 1] = degree * (degree + 1) / 4.0
    return derivative


def triple(table, rows):
    wide = np.zeros((rows, DEEP))
    wide[: table.shape[0], :FACE] = table
    high, low = halves(wide)
    return np.concatenate([high, high, low], axis=1)


def quadrature():
    degree = P_SIZE - 1
    points, values = lobatto(degree)
    return (points, 2.0 / (degree * (degree + 1) * values**2))


def tables():
    points, weights = quadrature()
    derivative = derivative_table()
    unit = np.eye(P_SIZE)
    near = [triple(t, SLAB) for t in (np.kron(derivative, unit), np.kron(unit, derivative))]
    coords = [c.reshape(-1) for c in np.meshgrid(points, points, indexing="ij")]
    face = np.outer(weights, weights).reshape(-1)
    even = np.zeros((24, FACE))
    uneven = np.zeros((24, FACE))
    for vertex in range(8):
        signs = [2.0 * (vertex >> 2 - m & 1) - 1.0 for m in range(3)]
        first, second = [(1.0 + signs[m + 1] * coords[m]) / 2.0 for m in range(2)]
        even[vertex] = signs[0] / 2.0 * first * second * face
        even[8 + vertex] = signs[1] / 4.0 * second * face
        even[16 + vertex] = signs[2] / 4.0 * first * face
        uneven[8 + vertex] = signs[0] * even[8 + vertex]
        uneven[16 + vertex] = signs[0] * even[16 + vertex]
    return np.concatenate([*near, triple(even, 32), triple(uneven, 32)], axis=0)


def face_weights(r, slots):
    points, weights = quadrature()
    face = np.outer(weights, weights).reshape(-1)
    row = lax.broadcasted_iota(jnp.int32, (8, slots), 0)
    value = jnp.zeros((8, slots), F32)
    for k, weight in enumerate(face[8 * r : 8 * r + 8]):
        value = jnp.where(row == k, float(weight), value)
    return value


def split(value):
    high = value.astype(BF16)
    return (high, (value - high.astype(F32)).astype(BF16))


def chunk(field, i, a, r):
    start = FACE * a + 8 * r
    if start + 8 <= NODES:
        return field[i, pl.ds(start, 8), :]
    rest = NODES - start
    row = lax.broadcasted_iota(jnp.int32, (8, field.shape[2]), 0)
    value = jnp.zeros((8, field.shape[2]), F32)
    for k in range(rest):
        value = jnp.where(row == k, field[i, pl.ds(start + k, 1), :], value)
    return value


def stacked(parts):
    high, low = split(jnp.concatenate(parts, axis=0))
    return jnp.concatenate([high, low, high], axis=0)


def near_derivatives(velocity, adjoint, table, near):
    blank = jnp.zeros((DEEP - SLAB, velocity.shape[2]), F32)
    for a in range(P_SIZE):
        fields = [
            stacked([*[chunk(field, i, a, r) for r in range(CHUNKS)], blank])
            for field in (velocity, adjoint)
            for i in range(3)
        ]
        near[a] = jnp.dot(
            table[: 2 * SLAB], jnp.concatenate(fields, axis=1), preferred_element_type=F32
        )


def far_derivatives(velocity, adjoint, far):
    table = derivative_table()
    for f in range(6):
        field = (velocity, adjoint)[f // 3]
        for r in range(CHUNKS):
            x = [chunk(field, f % 3, a, r) for a in range(P_SIZE)]
            plus = [x[j] + x[P_SIZE - 1 - j] for j in range(HALF)]
            minus = [x[j] - x[P_SIZE - 1 - j] for j in range(HALF)]

            def put(a, value):
                far[f, a, 8 * r : 8 * r + 8, :] = value

            for i in range(HALF):
                mirror = table[i, ::-1]
                even = float(table[i, HALF]) * x[HALF] + sum(
                    float(table[i, j] + mirror[j]) / 2.0 * plus[j] for j in range(HALF)
                )
                uneven = sum(float(table[i, j] - mirror[j]) / 2.0 * minus[j] for j in range(HALF))
                put(i, uneven + even)
                put(P_SIZE - 1 - i, uneven - even)
            put(HALF, sum(float(table[HALF, j]) * minus[j] for j in range(HALF)))


PAIRS = [(0, 1), (0, 2), (1, 2)]


def reduced(far, near, r, slots):
    points, weights = quadrature()

    def products(a):
        def grad(f, j):
            if j == 0:
                return far[f, a, 8 * r : 8 * r + 8, :]
            row = SLAB * (j - 1) + 8 * r
            return near[a, row : row + 8, f * slots : (f + 1) * slots]

        u = [[grad(i, j) for j in range(3)] for i in range(3)]
        w = [[grad(3 + i, j) for j in range(3)] for i in range(3)]
        stress = [sum(u[i][m] * w[i][m] for i in range(3)) for m in range(3)]
        stress += [
            sum(u[i][c] * w[i][j] for i in range(3)) + sum(w[i][c] * u[i][j] for i in range(3))
            for c, j in PAIRS
        ]
        return (stress, [sum(u[i][j] * u[i][j] for i in range(3)) for j in range(3)])

    stress, spent = products(HALF)
    even = [float(weights[HALF]) * s for s in stress]
    spent = [float(weights[HALF]) * s for s in spent]
    uneven = [None] * 6
    for a in range(HALF):
        here, here_spent = products(a)
        there, there_spent = products(P_SIZE - 1 - a)
        weight, moment = float(weights[a]), float(weights[a] * points[a])
        for k in range(6):
            even[k] = even[k] + weight * (here[k] + there[k])
            part = moment * (here[k] - there[k])
            uneven[k] = part if a == 0 else uneven[k] + part
        for k in range(3):
            spent[k] = spent[k] + weight * (here_spent[k] + there_spent[k])
    return (even, uneven, spent)


def element_terms(far, near, spacing, live, table):
    slots = spacing.shape[1]
    factor = [2.0 / spacing[j : j + 1] for j in range(3)]
    square = [f * f for f in factor]
    jacobian = spacing[0:1] * spacing[1:2] * spacing[2:3] * 0.125
    rows = [reduced(far, near, r, slots) for r in range(CHUNKS)]
    lost = 0.0
    for r in range(CHUNKS):
        level = sum(square[j] * rows[r][2][j] for j in range(3))
        lost = lost + face_weights(r, slots) * level
    blank = jnp.zeros((DEEP - SLAB, slots), F32)
    sums = 0.0
    for p in range(2):
        columns = [stacked([*[row[p][k] for row in rows], blank]) for k in range(6)]
        begin = 2 * SLAB + 32 * p
        sums = sums + jnp.dot(
            table[begin : begin + 32],
            jnp.concatenate(columns, axis=1),
            preferred_element_type=F32,
        )

    def part(j, column):
        return sums[8 * j : 8 * j + 8, column * slots : (column + 1) * slots]

    terms = []
    for c in range(3):
        total = sum(square[m] * part(c, m) for m in range(3)) - 2.0 * square[c] * part(c, c)
        for column, pair in enumerate(PAIRS):
            if c in pair:
                j = pair[0] + pair[1] - c
                total = total - square[j] * part(j, 3 + column)
        terms.append(jnp.where(live, total * (factor[c] * jacobian), 0.0))
    return (terms, jnp.where(live, lost * jacobian, 0.0))


def spread(row):
    return jnp.broadcast_to(row, (16, row.shape[1])).astype(BF16)


def place(index, rows, values=None):
    slots = index.shape[1]
    row = lax.broadcasted_iota(jnp.int32, (rows, slots), 0).astype(F32).astype(BF16)
    index = index.astype(F32)
    zero = jnp.zeros((rows, slots), BF16)
    columns = []
    for k in range(8):
        hit = row == jnp.concatenate([spread(index[k : k + 1])] * (rows // 16), axis=0)
        if values is None:
            columns.append(jnp.where(hit, jnp.ones_like(zero), zero))
        else:
            columns.append(
                jnp.concatenate([jnp.where(hit, spread(v[k : k + 1]), zero) for v in values], axis=0)
            )
    return jnp.concatenate(columns, axis=1)


def far_first(groups, grp):
    place = jnp.minimum(grp, groups - 1 - grp)
    sign = 1 - 2 * (2 * grp // groups)
    single = groups - 1 - 2 * place
    steps = []
    for turn in range(groups - 1):
        rest = turn - single
        pair = (place - rest // 2) * (1 - 2 * lax.rem(rest + 2 * groups, 2))
        offset = jnp.where(rest < 0, groups - 1 - place - turn, pair)
        steps.append(lax.rem(sign * offset + groups, groups))
    return steps


def kernel(
    groups, columns,
    velocity_in, adjoint_in, spacing_in, count_in, map_in, table_in,
    direction, objective,
    velocity, adjoint, spacing, count, design_map, table, near, far,
    outgoing, arrived, gathered_sums, gathered,
    local_sem, send_sem, recv_sem, hand_sem, send_all, recv_all,
):
    devices = groups * columns
    grp, col = lax.axis_index("grp"), lax.axis_index("elem")
    me = grp * columns + col
    slots = spacing.shape[1]

    barrier = pltpu.get_barrier_semaphore()
    pairs = [
        (velocity_in, velocity), (adjoint_in, adjoint), (table_in, table),
        (map_in, design_map), (spacing_in, spacing), (count_in, count),
    ]
    loads = [pltpu.make_async_copy(a, b, local_sem.at[i]) for i, (a, b) in enumerate(pairs)]
    for load in loads:
        load.start()

    steps = far_first(groups, grp)

    def at(step, turn):
        return (lax.rem(grp + step, groups), lax.rem(col + turn, columns))

    everyone = [(step, turn) for step in steps for turn in range(columns)]
    everyone += [(0, turn) for turn in range(1, columns)]
    for step, turn in everyone:
        pl.semaphore_signal(barrier, inc=1, device_id=at(step, turn), device_id_type=MESH)
    for load in loads[:3]:
        load.wait()

    near_derivatives(velocity, adjoint, table, near)
    far_derivatives(velocity, adjoint, far)

    for load in loads[3:]:
        load.wait()
    odd = lax.rem(col, 2)
    partner = col + 1 - 2 * odd
    outer = lax.rem(col + 2 * odd + columns - 1, columns)

    def message(slot, there, wait):
        return pltpu.make_async_remote_copy(
            src_ref=outgoing.at[0],
            dst_ref=arrived.at[slot],
            send_sem=send_sem,
            recv_sem=recv_sem.at[wait],
            device_id=there,
            device_id_type=MESH,
        )

    def arriving(slot, count, wait):
        part = arrived.at[pl.ds(slot, count)]
        return pltpu.make_async_remote_copy(
            src_ref=part,
            dst_ref=part,
            send_sem=hand_sem,
            recv_sem=recv_sem.at[wait],
            device_id=(grp, partner),
            device_id_type=MESH,
        )

    def pair(step):
        return arriving(along(0, step), 2, 2 + step)

    def whole(ref, count, semaphore):
        part = ref.at[pl.ds(0, count)]
        return pltpu.make_async_remote_copy(
            src_ref=part,
            dst_ref=part,
            send_sem=semaphore,
            recv_sem=semaphore,
            device_id=(grp, partner),
            device_id_type=MESH,
        )

    def along(parity, step):
        return groups + 2 * step - 1 + parity

    messages = []
    messages.append(message(0, (grp, partner), 0))
    messages.append(message(1, (grp, outer), 1))
    for step in steps:
        there = lax.rem(grp + step, groups)
        messages.append(message(along(odd, step), (there, col + 1 - odd), 2 + step))
        messages.append(message(1 + step, (there, outer), 2))

    live = lax.broadcasted_iota(jnp.int32, (8, slots), 1) < count[0]
    terms, spent = element_terms(far, near, spacing[...], live, table)
    for c in range(3):
        outgoing[0, 7 * c : 7 * c + 7, :] = terms[c][:7]
    outgoing[0, 21:29, :] = design_map[...].astype(F32)
    pl.semaphore_wait(barrier, devices - 1)
    for copy in messages:
        copy.start()

    base = me * UPPER

    def collect(blocks):
        uppers, lowers = [], []
        for ref, slot in blocks:
            nodes = ref[slot, 21:29, :].astype(jnp.int32)
            index = lax.shift_right_logical(nodes, jnp.full_like(nodes, LANES.bit_length() - 1)) - base
            highs, lows = [], []
            for c in range(3):
                term = ref[slot, 7 * c : 7 * c + 7, :]
                term = jnp.concatenate([term, -jnp.sum(term, axis=0, keepdims=True)], axis=0)
                highs.append(term.astype(BF16).astype(F32))
                lows.append(term - highs[c])
            uppers.append(place(index, UPPER, highs + lows))
            lowers.append(place(nodes & (LANES - 1), LANES))
        return lax.dot_general(
            jnp.concatenate(uppers, axis=1),
            jnp.concatenate(lowers, axis=1),
            (((1,), (1,)), ((), ())),
            preferred_element_type=F32,
        )

    edge = lax.rem(grp, groups - 1) == 0
    expected = [jnp.where(edge, a, b) for a, b in zip(steps, steps[::-1])]
    shared = [along(parity, step) for step in expected for parity in range(2)]
    direct = [1 + step for step in range(1, groups)]

    def add(slots_in):
        gathered_sums[...] += collect([(arrived, slot) for slot in slots_in])

    gathered[devices - 1, 1:2] = jnp.sum(spent, axis=0, keepdims=True)
    both = collect([(outgoing, 0)])
    arriving(0, 1, 0).wait_recv()
    gathered_sums[...] = both + collect([(arrived, 0)])

    @pl.when(odd == 1)
    def _():
        for step in expected:
            pair(step).wait_recv()
            pair(step).start()
        arriving(1, 1, 1).wait_recv()
        add([1, *shared])
        arriving(2, groups - 1, 2).wait_recv()
        add(direct)

    @pl.when(odd == 0)
    def _():
        arriving(1, 1, 1).wait_recv()
        add([1])
        arriving(2, groups - 1, 2).wait_recv()
        add(direct)
        for step in expected[:-1]:
            pair(step).wait_recv()
        add(shared[:-2])
        pair(expected[-1]).wait_recv()
        add(shared[-2:])

    both = gathered_sums[...]
    total = both[: 3 * UPPER] + both[3 * UPPER :]

    squares = total * total
    squares = sum(squares[8 * i : 8 * i + 8] for i in range(3 * UPPER // 8))
    gathered[devices - 1, 0:1] = jnp.sum(squares, axis=0, keepdims=True)

    def share(step, turn):
        slot = step * columns + turn - 1
        return pltpu.make_async_remote_copy(
            src_ref=gathered.at[devices - 1],
            dst_ref=gathered.at[slot],
            send_sem=send_all,
            recv_sem=recv_all,
            device_id=at(step, turn),
            device_id_type=MESH,
        )

    for step, turn in everyone:
        share(step, turn).start()
    whole(arrived, len(messages), send_sem).wait_send()
    whole(gathered, devices - 1, recv_all).wait_recv()
    everything = jnp.sum(gathered[...], axis=0)
    totals = jnp.sum(everything, axis=1, keepdims=True)
    square_total, spent_total = totals[:1], totals[1:]
    scale = lax.rsqrt(square_total * (1.0 / (3.0 * ND_DEV * devices)) + 1e-06)
    scaled = total * scale
    for c in range(3):
        direction[c] = scaled[UPPER * c : UPPER * c + UPPER]
    objective[...] = jnp.broadcast_to(spent_total * (1.0 / (NODES * slots * devices)), (1, LANES))
    whole(gathered, devices - 1, send_all).wait_send()

    @pl.when(odd == 1)
    def _():
        whole(arrived, 2 * (groups - 1), hand_sem).wait_send()


def hand_over(scaled, spent, direction, objective):
    for c in range(3):
        for u in range(UPPER):
            direction[c : c + 1, u * LANES : (u + 1) * LANES] = scaled[c, u : u + 1, :]
    objective[...] = spent[:, :1]


def body(groups, columns, velocity, adjoint, spacing, elem_count, design_map):
    devices = groups * columns
    blocks = 3 * groups
    slots = spacing.shape[1]
    vmem = pl.BlockSpec(memory_space=pltpu.VMEM)
    constant = tables()
    operands = [
        pltpu.with_memory_space_constraint(jnp.asarray(x), pltpu.HBM)
        for x in (velocity, adjoint, spacing)
    ]
    operands.append(elem_count)
    operands += [
        pltpu.with_memory_space_constraint(jnp.asarray(x), pltpu.HBM)
        for x in (design_map, constant)
    ]
    scaled, spent = pl.pallas_call(
        functools.partial(kernel, groups, columns),
        out_shape=(
            jax.ShapeDtypeStruct((3, UPPER, LANES), F32),
            jax.ShapeDtypeStruct((1, LANES), F32),
        ),
        in_specs=[pl.BlockSpec(memory_space=pltpu.HBM)] * 6,
        out_specs=(vmem, vmem),
        scratch_shapes=[
            pltpu.VMEM(velocity.shape, F32),
            pltpu.VMEM(adjoint.shape, F32),
            pltpu.VMEM(spacing.shape, F32),
            pltpu.SMEM((1,), jnp.int32),
            pltpu.VMEM((8, slots), jnp.int32),
            pltpu.VMEM(constant.shape, BF16),
            pltpu.VMEM((P_SIZE, 2 * SLAB, 6 * slots), F32),
            pltpu.VMEM((6, P_SIZE, SLAB, slots), F32),
            pltpu.VMEM((1, 29, slots), F32),
            pltpu.VMEM((blocks - 1, 29, slots), F32),
            pltpu.VMEM((6 * UPPER, LANES), F32),
            pltpu.VMEM((devices, 2, LANES), F32),
            pltpu.SemaphoreType.DMA((6,)),
            pltpu.SemaphoreType.DMA,
            pltpu.SemaphoreType.DMA((groups + 2,)),
            *[pltpu.SemaphoreType.DMA] * 3,
        ],
        compiler_params=pltpu.CompilerParams(
            collective_id=0, has_side_effects=True, vmem_limit_bytes=VMEM_BYTES
        ),
    )(*operands)
    direction, objective = pl.pallas_call(
        hand_over,
        out_shape=(
            jax.ShapeDtypeStruct((3, ND_DEV), F32),
            jax.ShapeDtypeStruct((1, 1), F32),
        ),
        in_specs=[vmem] * 2,
        out_specs=(vmem, vmem),
        compiler_params=pltpu.CompilerParams(vmem_limit_bytes=VMEM_BYTES),
    )(scaled, spent)
    return (direction, objective.reshape(()))


def solution(mesh):
    return jax.shard_map(
        functools.partial(body, mesh.shape["grp"], mesh.shape["elem"]),
        mesh=mesh,
        in_specs=(
            P(None, None, ("grp", "elem")),
            P(None, None, ("grp", "elem")),
            P(None, ("grp", "elem")),
            P(("grp", "elem")),
            P(None, ("grp", "elem")),
        ),
        out_specs=(P(None, ("grp", "elem")), P()),
        check_vma=False,
    )
```

```python
import functools

import jax
import jax.numpy as jnp
import numpy as np
from jax import lax
from jax.experimental import pallas as pl
from jax.experimental.pallas import tpu as pltpu
from jax.sharding import PartitionSpec as P

P_SIZE = 7
ND_DEV = 2048
LANES = 128
UPPER = ND_DEV // LANES
NODES = P_SIZE**3
FACE = P_SIZE * P_SIZE
CHUNKS = -(-FACE // 8)
SLAB = 8 * CHUNKS
DEEP = 64
HALF = P_SIZE // 2
MESH = pl.DeviceIdType.MESH
F32 = jnp.float32
BF16 = jnp.bfloat16
VMEM_BYTES = 32 * 2**20


def lobatto(degree):
    points = np.cos(np.pi * np.arange(degree + 1) / degree)
    for sweep in range(60):
        lower = np.ones(degree + 1)
        upper = points.copy()
        for order in range(2, degree + 1):
            lower, upper = (upper, ((2 * order - 1) * points * upper - (order - 1) * lower) / order)
        points = points - (points * upper - lower) / ((degree + 1) * upper)
    lower = np.ones(degree + 1)
    upper = points.copy()
    for order in range(2, degree + 1):
        lower, upper = (upper, ((2 * order - 1) * points * upper - (order - 1) * lower) / order)
    return (points[::-1].copy(), upper[::-1].copy())


def halves(table):
    exact = np.asarray(table, np.float32)
    high = exact.astype(BF16)
    low = (exact - high.astype(np.float32)).astype(BF16)
    return (high, low)


def derivative_table():
    degree = P_SIZE - 1
    points, values = lobatto(degree)
    derivative = np.zeros((P_SIZE, P_SIZE))
    for i in range(P_SIZE):
        for j in range(P_SIZE):
            if i != j:
                derivative[i, j] = values[i] / (values[j] * (points[i] - points[j]))
    derivative[0, 0] = -degree * (degree + 1) / 4.0
    derivative[P_SIZE - 1, P_SIZE - 1] = degree * (degree + 1) / 4.0
    return derivative


def triple(table, rows):
    wide = np.zeros((rows, DEEP))
    wide[: table.shape[0], :FACE] = table
    high, low = halves(wide)
    return np.concatenate([high, high, low], axis=1)


def quadrature():
    degree = P_SIZE - 1
    points, values = lobatto(degree)
    return (points, 2.0 / (degree * (degree + 1) * values**2))


def tables():
    points, weights = quadrature()
    derivative = derivative_table()
    unit = np.eye(P_SIZE)
    near = [triple(t, SLAB) for t in (np.kron(derivative, unit), np.kron(unit, derivative))]
    coords = [c.reshape(-1) for c in np.meshgrid(points, points, indexing="ij")]
    face = np.outer(weights, weights).reshape(-1)
    even = np.zeros((24, FACE))
    uneven = np.zeros((24, FACE))
    for vertex in range(8):
        signs = [2.0 * (vertex >> 2 - m & 1) - 1.0 for m in range(3)]
        first, second = [(1.0 + signs[m + 1] * coords[m]) / 2.0 for m in range(2)]
        even[vertex] = signs[0] / 2.0 * first * second * face
        even[8 + vertex] = signs[1] / 4.0 * second * face
        even[16 + vertex] = signs[2] / 4.0 * first * face
        uneven[8 + vertex] = signs[0] * even[8 + vertex]
        uneven[16 + vertex] = signs[0] * even[16 + vertex]
    return np.concatenate([*near, triple(even, 32), triple(uneven, 32)], axis=0)


def face_weights(r, slots):
    points, weights = quadrature()
    face = np.outer(weights, weights).reshape(-1)
    row = lax.broadcasted_iota(jnp.int32, (8, slots), 0)
    value = jnp.zeros((8, slots), F32)
    for k, weight in enumerate(face[8 * r : 8 * r + 8]):
        value = jnp.where(row == k, float(weight), value)
    return value


def split(value):
    high = value.astype(BF16)
    return (high, (value - high.astype(F32)).astype(BF16))


def chunk(field, i, a, r):
    start = FACE * a + 8 * r
    if start + 8 <= NODES:
        return field[i, pl.ds(start, 8), :]
    rest = NODES - start
    row = lax.broadcasted_iota(jnp.int32, (8, field.shape[2]), 0)
    value = jnp.zeros((8, field.shape[2]), F32)
    for k in range(rest):
        value = jnp.where(row == k, field[i, pl.ds(start + k, 1), :], value)
    return value


def stacked(parts):
    high, low = split(jnp.concatenate(parts, axis=0))
    return jnp.concatenate([high, low, high], axis=0)


def near_derivatives(velocity, adjoint, table, near):
    blank = jnp.zeros((DEEP - SLAB, velocity.shape[2]), F32)
    for a in range(P_SIZE):
        fields = [
            stacked([*[chunk(field, i, a, r) for r in range(CHUNKS)], blank])
            for field in (velocity, adjoint)
            for i in range(3)
        ]
        near[a] = jnp.dot(
            table[: 2 * SLAB], jnp.concatenate(fields, axis=1), preferred_element_type=F32
        )


def far_derivatives(velocity, adjoint, far):
    table = derivative_table()
    for f in range(6):
        field = (velocity, adjoint)[f // 3]
        for r in range(CHUNKS):
            x = [chunk(field, f % 3, a, r) for a in range(P_SIZE)]
            plus = [x[j] + x[P_SIZE - 1 - j] for j in range(HALF)]
            minus = [x[j] - x[P_SIZE - 1 - j] for j in range(HALF)]

            def put(a, value):
                far[f, a, 8 * r : 8 * r + 8, :] = value

            for i in range(HALF):
                mirror = table[i, ::-1]
                even = float(table[i, HALF]) * x[HALF] + sum(
                    float(table[i, j] + mirror[j]) / 2.0 * plus[j] for j in range(HALF)
                )
                uneven = sum(float(table[i, j] - mirror[j]) / 2.0 * minus[j] for j in range(HALF))
                put(i, uneven + even)
                put(P_SIZE - 1 - i, uneven - even)
            put(HALF, sum(float(table[HALF, j]) * minus[j] for j in range(HALF)))


PAIRS = [(0, 1), (0, 2), (1, 2)]


def reduced(far, near, r, slots):
    points, weights = quadrature()

    def products(a):
        def grad(f, j):
            if j == 0:
                return far[f, a, 8 * r : 8 * r + 8, :]
            row = SLAB * (j - 1) + 8 * r
            return near[a, row : row + 8, f * slots : (f + 1) * slots]

        u = [[grad(i, j) for j in range(3)] for i in range(3)]
        w = [[grad(3 + i, j) for j in range(3)] for i in range(3)]
        stress = [sum(u[i][m] * w[i][m] for i in range(3)) for m in range(3)]
        stress += [
            sum(u[i][c] * w[i][j] for i in range(3)) + sum(w[i][c] * u[i][j] for i in range(3))
            for c, j in PAIRS
        ]
        return (stress, [sum(u[i][j] * u[i][j] for i in range(3)) for j in range(3)])

    stress, spent = products(HALF)
    even = [float(weights[HALF]) * s for s in stress]
    spent = [float(weights[HALF]) * s for s in spent]
    uneven = [None] * 6
    for a in range(HALF):
        here, here_spent = products(a)
        there, there_spent = products(P_SIZE - 1 - a)
        weight, moment = float(weights[a]), float(weights[a] * points[a])
        for k in range(6):
            even[k] = even[k] + weight * (here[k] + there[k])
            part = moment * (here[k] - there[k])
            uneven[k] = part if a == 0 else uneven[k] + part
        for k in range(3):
            spent[k] = spent[k] + weight * (here_spent[k] + there_spent[k])
    return (even, uneven, spent)


def element_terms(far, near, spacing, live, table):
    slots = spacing.shape[1]
    factor = [2.0 / spacing[j : j + 1] for j in range(3)]
    square = [f * f for f in factor]
    jacobian = spacing[0:1] * spacing[1:2] * spacing[2:3] * 0.125
    rows = [reduced(far, near, r, slots) for r in range(CHUNKS)]
    lost = 0.0
    for r in range(CHUNKS):
        level = sum(square[j] * rows[r][2][j] for j in range(3))
        lost = lost + face_weights(r, slots) * level
    blank = jnp.zeros((DEEP - SLAB, slots), F32)
    sums = 0.0
    for p in range(2):
        columns = [stacked([*[row[p][k] for row in rows], blank]) for k in range(6)]
        begin = 2 * SLAB + 32 * p
        sums = sums + jnp.dot(
            table[begin : begin + 32],
            jnp.concatenate(columns, axis=1),
            preferred_element_type=F32,
        )

    def part(j, column):
        return sums[8 * j : 8 * j + 8, column * slots : (column + 1) * slots]

    terms = []
    for c in range(3):
        total = sum(square[m] * part(c, m) for m in range(3)) - 2.0 * square[c] * part(c, c)
        for column, pair in enumerate(PAIRS):
            if c in pair:
                j = pair[0] + pair[1] - c
                total = total - square[j] * part(j, 3 + column)
        terms.append(jnp.where(live, total * (factor[c] * jacobian), 0.0))
    return (terms, jnp.where(live, lost * jacobian, 0.0))


def spread(row):
    return jnp.broadcast_to(row, (16, row.shape[1])).astype(BF16)


def place(index, rows, values=None):
    slots = index.shape[1]
    row = lax.broadcasted_iota(jnp.int32, (rows, slots), 0).astype(F32).astype(BF16)
    index = index.astype(F32)
    zero = jnp.zeros((rows, slots), BF16)
    columns = []
    for k in range(8):
        hit = row == jnp.concatenate([spread(index[k : k + 1])] * (rows // 16), axis=0)
        if values is None:
            columns.append(jnp.where(hit, jnp.ones_like(zero), zero))
        else:
            columns.append(
                jnp.concatenate([jnp.where(hit, spread(v[k : k + 1]), zero) for v in values], axis=0)
            )
    return jnp.concatenate(columns, axis=1)


def far_first(groups, grp):
    place = jnp.minimum(grp, groups - 1 - grp)
    sign = 1 - 2 * (2 * grp // groups)
    single = groups - 1 - 2 * place
    steps = []
    for turn in range(groups - 1):
        rest = turn - single
        pair = (place - rest // 2) * (1 - 2 * lax.rem(rest + 2 * groups, 2))
        offset = jnp.where(rest < 0, groups - 1 - place - turn, pair)
        steps.append(lax.rem(sign * offset + groups, groups))
    return steps


def kernel(
    groups, columns,
    velocity_in, adjoint_in, spacing_in, count_in, map_in, table_in,
    direction, objective,
    velocity, adjoint, spacing, count, design_map, table, near, far,
    outgoing, arrived, gathered_sums, gathered,
    local_sem, send_sem, recv_sem, hand_sem, send_all, recv_all,
):
    devices = groups * columns
    grp, col = lax.axis_index("grp"), lax.axis_index("elem")
    me = grp * columns + col
    slots = spacing.shape[1]

    barrier = pltpu.get_barrier_semaphore()
    pairs = [
        (velocity_in, velocity), (adjoint_in, adjoint), (table_in, table),
        (map_in, design_map), (spacing_in, spacing), (count_in, count),
    ]
    steps = far_first(groups, grp)

    def at(step, turn):
        return (lax.rem(grp + step, groups), lax.rem(col + turn, columns))

    everyone = [(step, turn) for step in steps for turn in range(columns)]
    everyone += [(0, turn) for turn in range(1, columns)]
    for step, turn in everyone[:columns]:
        pl.semaphore_signal(barrier, inc=1, device_id=at(step, turn), device_id_type=MESH)
    loads = [pltpu.make_async_copy(a, b, local_sem.at[i]) for i, (a, b) in enumerate(pairs)]
    for load in loads:
        load.start()

    for step, turn in everyone[columns:]:
        pl.semaphore_signal(barrier, inc=1, device_id=at(step, turn), device_id_type=MESH)
    for load in loads[:3]:
        load.wait()

    near_derivatives(velocity, adjoint, table, near)
    far_derivatives(velocity, adjoint, far)

    for load in loads[3:]:
        load.wait()
    odd = lax.rem(col, 2)
    partner = col + 1 - 2 * odd
    outer = lax.rem(col + 2 * odd + columns - 1, columns)

    def message(slot, there, wait):
        return pltpu.make_async_remote_copy(
            src_ref=outgoing.at[0],
            dst_ref=arrived.at[slot],
            send_sem=send_sem,
            recv_sem=recv_sem.at[wait],
            device_id=there,
            device_id_type=MESH,
        )

    def arriving(slot, count, wait):
        part = arrived.at[pl.ds(slot, count)]
        return pltpu.make_async_remote_copy(
            src_ref=part,
            dst_ref=part,
            send_sem=hand_sem,
            recv_sem=recv_sem.at[wait],
            device_id=(grp, partner),
            device_id_type=MESH,
        )

    def pair(step):
        return arriving(along(0, step), 2, 2 + step)

    def whole(ref, count, semaphore):
        part = ref.at[pl.ds(0, count)]
        return pltpu.make_async_remote_copy(
            src_ref=part,
            dst_ref=part,
            send_sem=semaphore,
            recv_sem=semaphore,
            device_id=(grp, partner),
            device_id_type=MESH,
        )

    def along(parity, step):
        return groups + 2 * step - 1 + parity

    messages = []
    messages.append(message(0, (grp, partner), 0))
    messages.append(message(1, (grp, outer), 1))
    for step in steps:
        there = lax.rem(grp + step, groups)
        messages.append(message(along(odd, step), (there, col + 1 - odd), 2 + step))
        messages.append(message(1 + step, (there, outer), 2))

    live = lax.broadcasted_iota(jnp.int32, (8, slots), 1) < count[0]
    terms, spent = element_terms(far, near, spacing[...], live, table)
    for c in range(3):
        outgoing[0, 7 * c : 7 * c + 7, :] = terms[c][:7]
    outgoing[0, 21:29, :] = design_map[...].astype(F32)
    pl.semaphore_wait(barrier, devices - 1)
    for copy in messages:
        copy.start()

    base = me * UPPER

    def collect(blocks):
        uppers, lowers = [], []
        for ref, slot in blocks:
            nodes = ref[slot, 21:29, :].astype(jnp.int32)
            index = lax.shift_right_logical(nodes, jnp.full_like(nodes, LANES.bit_length() - 1)) - base
            highs, lows = [], []
            for c in range(3):
                term = ref[slot, 7 * c : 7 * c + 7, :]
                term = jnp.concatenate([term, -jnp.sum(term, axis=0, keepdims=True)], axis=0)
                highs.append(term.astype(BF16).astype(F32))
                lows.append(term - highs[c])
            uppers.append(place(index, UPPER, highs + lows))
            lowers.append(place(nodes & (LANES - 1), LANES))
        return lax.dot_general(
            jnp.concatenate(uppers, axis=1),
            jnp.concatenate(lowers, axis=1),
            (((1,), (1,)), ((), ())),
            preferred_element_type=F32,
        )

    edge = lax.rem(grp, groups - 1) == 0
    expected = [jnp.where(edge, a, b) for a, b in zip(steps, steps[::-1])]
    shared = [along(parity, step) for step in expected for parity in range(2)]
    direct = [1 + step for step in range(1, groups)]

    def add(slots_in):
        gathered_sums[...] += collect([(arrived, slot) for slot in slots_in])

    gathered[devices - 1, 1:2] = jnp.sum(spent, axis=0, keepdims=True)
    both = collect([(outgoing, 0)])
    arriving(0, 1, 0).wait_recv()
    gathered_sums[...] = both + collect([(arrived, 0)])

    @pl.when(odd == 1)
    def _():
        for step in expected:
            pair(step).wait_recv()
            pair(step).start()
        arriving(1, 1, 1).wait_recv()
        add([1, *shared])
        arriving(2, groups - 1, 2).wait_recv()
        add(direct)

    @pl.when(odd == 0)
    def _():
        arriving(1, 1, 1).wait_recv()
        add([1])
        arriving(2, groups - 1, 2).wait_recv()
        add(direct)
        for step in expected[:-1]:
            pair(step).wait_recv()
        add(shared[:-2])
        pair(expected[-1]).wait_recv()
        add(shared[-2:])

    both = gathered_sums[...]
    total = both[: 3 * UPPER] + both[3 * UPPER :]

    squares = total * total
    squares = sum(squares[8 * i : 8 * i + 8] for i in range(3 * UPPER // 8))
    gathered[devices - 1, 0:1] = jnp.sum(squares, axis=0, keepdims=True)

    def share(step, turn):
        slot = step * columns + turn - 1
        return pltpu.make_async_remote_copy(
            src_ref=gathered.at[devices - 1],
            dst_ref=gathered.at[slot],
            send_sem=send_all,
            recv_sem=recv_all,
            device_id=at(step, turn),
            device_id_type=MESH,
        )

    for step, turn in everyone:
        share(step, turn).start()
    whole(arrived, len(messages), send_sem).wait_send()
    @pl.when(odd == 1)
    def _():
        whole(arrived, 2 * (groups - 1), hand_sem).wait_send()

    whole(gathered, devices - 1, send_all).wait_send()
    whole(gathered, devices - 1, recv_all).wait_recv()
    everything = jnp.sum(gathered[...], axis=0)
    totals = jnp.sum(everything, axis=1, keepdims=True)
    square_total, spent_total = totals[:1], totals[1:]
    scale = lax.rsqrt(square_total * (1.0 / (3.0 * ND_DEV * devices)) + 1e-06)
    scaled = total * scale
    for c in range(3):
        direction[c] = scaled[UPPER * c : UPPER * c + UPPER]
    objective[...] = jnp.broadcast_to(spent_total * (1.0 / (NODES * slots * devices)), (1, LANES))


def hand_over(scaled, spent, direction, objective):
    for c in range(3):
        for u in range(UPPER):
            direction[c : c + 1, u * LANES : (u + 1) * LANES] = scaled[c, u : u + 1, :]
    objective[...] = spent[:, :1]


def body(groups, columns, velocity, adjoint, spacing, elem_count, design_map):
    devices = groups * columns
    blocks = 3 * groups
    slots = spacing.shape[1]
    vmem = pl.BlockSpec(memory_space=pltpu.VMEM)
    constant = tables()
    operands = [
        pltpu.with_memory_space_constraint(jnp.asarray(x), pltpu.HBM)
        for x in (velocity, adjoint, spacing)
    ]
    operands.append(elem_count)
    operands += [
        pltpu.with_memory_space_constraint(jnp.asarray(x), pltpu.HBM)
        for x in (design_map, constant)
    ]
    scaled, spent = pl.pallas_call(
        functools.partial(kernel, groups, columns),
        out_shape=(
            jax.ShapeDtypeStruct((3, UPPER, LANES), F32),
            jax.ShapeDtypeStruct((1, LANES), F32),
        ),
        in_specs=[pl.BlockSpec(memory_space=pltpu.HBM)] * 6,
        out_specs=(vmem, vmem),
        scratch_shapes=[
            pltpu.VMEM(velocity.shape, F32),
            pltpu.VMEM(adjoint.shape, F32),
            pltpu.VMEM(spacing.shape, F32),
            pltpu.SMEM((1,), jnp.int32),
            pltpu.VMEM((8, slots), jnp.int32),
            pltpu.VMEM(constant.shape, BF16),
            pltpu.VMEM((P_SIZE, 2 * SLAB, 6 * slots), F32),
            pltpu.VMEM((6, P_SIZE, SLAB, slots), F32),
            pltpu.VMEM((1, 29, slots), F32),
            pltpu.VMEM((blocks - 1, 29, slots), F32),
            pltpu.VMEM((6 * UPPER, LANES), F32),
            pltpu.VMEM((devices, 2, LANES), F32),
            pltpu.SemaphoreType.DMA((6,)),
            pltpu.SemaphoreType.DMA,
            pltpu.SemaphoreType.DMA((groups + 2,)),
            *[pltpu.SemaphoreType.DMA] * 3,
        ],
        compiler_params=pltpu.CompilerParams(
            collective_id=0, has_side_effects=True, vmem_limit_bytes=VMEM_BYTES
        ),
    )(*operands)
    direction, objective = pl.pallas_call(
        hand_over,
        out_shape=(
            jax.ShapeDtypeStruct((3, ND_DEV), F32),
            jax.ShapeDtypeStruct((1, 1), F32),
        ),
        in_specs=[vmem] * 2,
        out_specs=(vmem, vmem),
        compiler_params=pltpu.CompilerParams(vmem_limit_bytes=VMEM_BYTES),
    )(scaled, spent)
    return (direction, objective.reshape(()))


def solution(mesh):
    return jax.shard_map(
        functools.partial(body, mesh.shape["grp"], mesh.shape["elem"]),
        mesh=mesh,
        in_specs=(
            P(None, None, ("grp", "elem")),
            P(None, None, ("grp", "elem")),
            P(None, ("grp", "elem")),
            P(("grp", "elem")),
            P(None, ("grp", "elem")),
        ),
        out_specs=(P(None, ("grp", "elem")), P()),
        check_vma=False,
    )
```
